128 devices in a mesh: group: 4 (over y_hi, core), patch: 32 (over y_lo, x, z).
Axes of the slice: x: 4, y: 4 (y_hi: 2, y_lo: 2; y = y_hi * 2 + y_lo), z: 4, core: 2. Of those that a mesh axis runs over, the one named last changes fastest.
Arguments:
- fine_nodes: bfloat16 [131072, 512], P(('group', 'patch')), may hold values from -6 to 6
- coarse_nodes: bfloat16 [2048, 512], P(('group', 'patch')), may hold values from -6 to 6
- fine_edges: bfloat16 [524288, 512], P(('group', 'patch')), may hold values from -6 to 6
- fine_senders: int32 [524288], P(('group', 'patch')), may hold values from 0 to 1279
- fine_receivers: int32 [524288], P(('group', 'patch')), may hold values from 0 to 1023
- fine_live: int32 [128], P(('group', 'patch')), may hold values from 128 to 4096, as said below
- up_edges: bfloat16 [65536, 512], P(('group', 'patch')), may hold values from -6 to 6
- up_senders: int32 [65536], P(('group', 'patch')), may hold values from 0 to 1023
- up_receivers: int32 [65536], P(('group', 'patch')), may hold values from 0 to 2047
- down_edges: bfloat16 [65536, 512], P(('group', 'patch')), may hold values from -6 to 6
- down_senders: int32 [65536], P(('group', 'patch')), may hold values from 0 to 2047
- down_receivers: int32 [65536], P(('group', 'patch')), may hold values from 0 to 1023
- edge_in_weight: bfloat16 [1536, 512], replicated, may hold values from -0.15625 to 0.15625
- edge_in_bias: float32 [512], replicated, may hold values from -3 to 3
- edge_out_weight: bfloat16 [512, 512], replicated, may hold values from -0.25 to 0.25
- edge_out_bias: float32 [512], replicated, may hold values from -3 to 3
- edge_gain: float32 [512], replicated, may hold values from 0.25 to 1.75
- edge_shift: float32 [512], replicated, may hold values from -2 to 2
- node_in_weight: bfloat16 [1024, 512], replicated, may hold values from -0.1875 to 0.1875
- node_in_bias: float32 [512], replicated, may hold values from -3 to 3
- node_out_weight: bfloat16 [512, 512], replicated, may hold values from -0.25 to 0.25
- node_out_bias: float32 [512], replicated, may hold values from -3 to 3
- node_gain: float32 [512], replicated, may hold values from 0.25 to 1.75
- node_shift: float32 [512], replicated, may hold values from -2 to 2
Outputs:
- fine_out: bfloat16 [131072, 512], P(('group', 'patch'))
- coarse_out: bfloat16 [2048, 512], P(('group', 'patch'))
- fine_edges_out: bfloat16 [524288, 512], P(('group', 'patch'))
- up_edges_out: bfloat16 [65536, 512], P(('group', 'patch'))
- down_edges_out: bfloat16 [65536, 512], P(('group', 'patch'))
The draws below stay inside these ranges and needn't reach their ends.
Inputs may be any that keep to these rules, and one draw needn't show every extreme that they name: `fine_live`: a multiple of 128; some patch has all 4096 slots live in every draw.
All inputs are finite; a program needn't handle non-finite values.
Results may differ from the reference program's by a relative error of at most 0.0049.
Values may be sent and summed in bfloat16 or wider, within the bound.
A program may use at most 128 MiB of HBM per device.

```python
import jax
import jax.numpy as jnp
from jax import lax

L = 512
NODE_DEV = 1024
RIM = 128
FE_DEV = 4096
EBLK = 128
UE_DEV = 512
DE_DEV = 512
FBLK = 32
NODES = 131072
COARSE = 2048
FINE_EDGES = 524288
UP_EDGES = 65536
DOWN_EDGES = 65536
N_GROUP = 4
N_PATCH = 32
DEVICES = 128


def draw_fine_live(key, part):
    blocks = jax.random.randint(jax.random.fold_in(key, 11), (DEVICES,), 1, FBLK + 1)
    chosen = jax.random.randint(jax.random.fold_in(key, 12), (), 0, DEVICES)
    blocks = jnp.where(jnp.arange(DEVICES) == chosen, FBLK, blocks)
    return (blocks * EBLK).astype(jnp.int32)


def touch_ends(drawn, stream_key, smallest, largest):
    longest = drawn.shape.index(max(drawn.shape))
    spots = []
    for shift in (0, 1):
        where = [jax.random.randint(jax.random.fold_in(stream_key, axis), (), 0, length) for axis, length in enumerate(drawn.shape)]
        where[longest] = (where[longest] + shift) % drawn.shape[longest]
        spots.append(tuple(where))
    return drawn.at[spots[0]].set(smallest).at[spots[1]].set(largest)


def shard_levels(stream_key, dims, shards, smallest, largest):
    loudness = 1.0
    for position, blocks in shards:
        steps = jax.random.uniform(jax.random.fold_in(jax.random.fold_in(stream_key, 6), position), (blocks,), jnp.float32, smallest / len(shards), largest / len(shards))
        loudness = loudness * jnp.repeat(jnp.exp(steps), dims[position] // blocks).reshape((-1,) + (1,) * (len(dims) - 1 - position))
    return loudness


def normal_values(key, shape, deviation, most, split=(), dtype=jnp.bfloat16):
    values = deviation * jax.random.normal(key, shape, jnp.float32)
    if split:
        values = values * shard_levels(key, shape, split, -0.22, 0.18)
    return jnp.clip(values, -most, most).astype(dtype)


def setup_inputs(seed: int = 0) -> dict:
    key_of = jax.random.split(jax.random.key(seed), 25)
    return {
        "fine_nodes": normal_values(key_of[0], (NODES, L), 1.0, 6.0, ((0, 128),)),
        "coarse_nodes": normal_values(key_of[1], (COARSE, L), 1.0, 6.0, ((0, 128),)),
        "fine_edges": normal_values(key_of[2], (FINE_EDGES, L), 1.0, 6.0, ((0, 128),)),
        "fine_senders": touch_ends(jax.random.randint(key_of[3], (FINE_EDGES,), 0, NODE_DEV + 2 * RIM), jax.random.fold_in(key_of[3], 1), 0, (NODE_DEV + 2 * RIM) - 1).astype(jnp.int32),
        "fine_receivers": touch_ends(jax.random.randint(key_of[4], (FINE_EDGES,), 0, NODE_DEV), jax.random.fold_in(key_of[4], 1), 0, NODE_DEV - 1).astype(jnp.int32),
        "fine_live": draw_fine_live(jax.random.fold_in(key_of[24], 71), 0),
        "up_edges": normal_values(key_of[6], (UP_EDGES, L), 1.0, 6.0, ((0, 128),)),
        "up_senders": touch_ends(jax.random.randint(key_of[7], (UP_EDGES,), 0, NODE_DEV), jax.random.fold_in(key_of[7], 1), 0, NODE_DEV - 1).astype(jnp.int32),
        "up_receivers": touch_ends(jax.random.randint(key_of[8], (UP_EDGES,), 0, COARSE), jax.random.fold_in(key_of[8], 1), 0, COARSE - 1).astype(jnp.int32),
        "down_edges": normal_values(key_of[9], (DOWN_EDGES, L), 1.0, 6.0, ((0, 128),)),
        "down_senders": touch_ends(jax.random.randint(key_of[10], (DOWN_EDGES,), 0, COARSE), jax.random.fold_in(key_of[10], 1), 0, COARSE - 1).astype(jnp.int32),
        "down_receivers": touch_ends(jax.random.randint(key_of[11], (DOWN_EDGES,), 0, NODE_DEV), jax.random.fold_in(key_of[11], 1), 0, NODE_DEV - 1).astype(jnp.int32),
        "edge_in_weight": normal_values(key_of[12], (3 * L, L), (3 * L) ** -0.5, 0.15625),
        "edge_in_bias": normal_values(key_of[13], (L,), 0.5, 3.0, (), jnp.float32),
        "edge_out_weight": normal_values(key_of[14], (L, L), L ** -0.5, 0.25),
        "edge_out_bias": normal_values(key_of[15], (L,), 0.5, 3.0, (), jnp.float32),
        "edge_gain": jnp.clip(1.0 + 0.15 * jax.random.normal(key_of[16], (L,), jnp.float32), 0.25, 1.75),
        "edge_shift": normal_values(key_of[17], (L,), 0.3, 2.0, (), jnp.float32),
        "node_in_weight": normal_values(key_of[18], (2 * L, L), (2 * L) ** -0.5, 0.1875),
        "node_in_bias": normal_values(key_of[19], (L,), 0.5, 3.0, (), jnp.float32),
        "node_out_weight": normal_values(key_of[20], (L, L), L ** -0.5, 0.25),
        "node_out_bias": normal_values(key_of[21], (L,), 0.5, 3.0, (), jnp.float32),
        "node_gain": jnp.clip(1.0 + 0.15 * jax.random.normal(key_of[22], (L,), jnp.float32), 0.25, 1.75),
        "node_shift": normal_values(key_of[23], (L,), 0.3, 2.0, (), jnp.float32),
    }


def perceptron(inputs, in_weight, in_bias, out_weight, out_bias, gain, shift):
    preact = jnp.dot(inputs, in_weight, preferred_element_type=jnp.float32) + in_bias.astype(jnp.float32)
    hidden = jax.nn.silu(preact).astype(jnp.bfloat16)
    result = jnp.dot(hidden, out_weight, preferred_element_type=jnp.float32) + out_bias.astype(jnp.float32)
    average = lax.optimization_barrier(jnp.mean(result, axis=-1, keepdims=True))
    centred = result - average
    spread = lax.optimization_barrier(jnp.mean(centred * centred, axis=-1, keepdims=True))
    return centred * lax.rsqrt(spread + 1e-05) * gain.astype(jnp.float32) + shift.astype(jnp.float32)

def reference(fine_nodes, coarse_nodes, fine_edges, fine_senders, fine_receivers, fine_live, up_edges, up_senders, up_receivers, down_edges, down_senders, down_receivers, edge_in_weight, edge_in_bias, edge_out_weight, edge_out_bias, edge_gain, edge_shift, node_in_weight, node_in_bias, node_out_weight, node_out_bias, node_gain, node_shift):
    edge_params = (edge_in_weight, edge_in_bias, edge_out_weight, edge_out_bias, edge_gain, edge_shift)
    node_params = (node_in_weight, node_in_bias, node_out_weight, node_out_bias, node_gain, node_shift)
    node_grid = fine_nodes.reshape(N_GROUP, N_PATCH, NODE_DEV, L)
    before_rim = jnp.roll(node_grid, 1, axis=1)[:, :, NODE_DEV - RIM:]
    after_rim = jnp.roll(node_grid, -1, axis=1)[:, :, :RIM]
    windows = jnp.concatenate([before_rim, node_grid, after_rim], axis=2).reshape(DEVICES, NODE_DEV + 2 * RIM, L)
    pieces = (windows, fine_edges.reshape(DEVICES, FE_DEV, L), fine_senders.reshape(DEVICES, FE_DEV), fine_receivers.reshape(DEVICES, FE_DEV), fine_live, up_edges.reshape(DEVICES, UE_DEV, L), up_senders.reshape(DEVICES, UE_DEV), up_receivers.reshape(DEVICES, UE_DEV), down_edges.reshape(DEVICES, DE_DEV, L), down_senders.reshape(DEVICES, DE_DEV), down_receivers.reshape(DEVICES, DE_DEV))

    def device_step(coarse_total, piece):
        window, f_edges, f_send, f_recv, live, u_edges, u_send, u_recv, d_edges, d_send, d_recv = piece
        owned_rows = window[RIM:RIM + NODE_DEV]
        fine_in = jnp.concatenate([f_edges, window[f_send], owned_rows[f_recv]], axis=1)
        fine_new = f_edges.astype(jnp.float32) + perceptron(fine_in, *edge_params)
        live_mask = (jnp.arange(FE_DEV) < live)[:, None]
        fine_new = jnp.where(live_mask, fine_new, f_edges.astype(jnp.float32))
        up_in = jnp.concatenate([u_edges, owned_rows[u_send], coarse_nodes[u_recv]], axis=1)
        up_new = u_edges.astype(jnp.float32) + perceptron(up_in, *edge_params)
        down_in = jnp.concatenate([d_edges, coarse_nodes[d_send], owned_rows[d_recv]], axis=1)
        down_new = d_edges.astype(jnp.float32) + perceptron(down_in, *edge_params)
        fine_sum = jax.ops.segment_sum(jnp.where(live_mask, fine_new, 0.0), f_recv, num_segments=NODE_DEV)
        fine_sum = (fine_sum + jax.ops.segment_sum(down_new, d_recv, num_segments=NODE_DEV)).astype(jnp.bfloat16)
        node_new = owned_rows.astype(jnp.float32) + perceptron(jnp.concatenate([owned_rows, fine_sum], axis=1), *node_params)
        coarse_total = coarse_total + jax.ops.segment_sum(up_new, u_recv, num_segments=COARSE)
        return (coarse_total, (node_new.astype(jnp.bfloat16), fine_new.astype(jnp.bfloat16), up_new.astype(jnp.bfloat16), down_new.astype(jnp.bfloat16)))
    coarse_total, outputs = lax.scan(device_step, jnp.zeros((COARSE, L), jnp.float32), pieces)
    coarse_sum = coarse_total.astype(jnp.bfloat16)
    coarse_out = coarse_nodes.astype(jnp.float32) + perceptron(jnp.concatenate([coarse_nodes, coarse_sum], axis=1), *node_params)
    return (outputs[0].reshape(NODES, L), coarse_out.astype(jnp.bfloat16), outputs[1].reshape(FINE_EDGES, L), outputs[2].reshape(UP_EDGES, L), outputs[3].reshape(DOWN_EDGES, L))
```

```python
import functools

import jax
import jax.numpy as jnp
from jax import lax
from jax.experimental import pallas as pl
from jax.experimental.pallas import tpu as pltpu
from jax.sharding import PartitionSpec as P

RIM = 128
BF = jnp.bfloat16
F32 = jnp.float32
TILE = 1024
BOTH = ("group", "patch")


def dot(a, b):
    return jnp.dot(a, b, preferred_element_type=F32)


def dot_t(a, b):
    return lax.dot_general(a, b, (((0,), (0,)), ((), ())), preferred_element_type=F32)


def one_hot_t(rows, index):
    iota = lax.broadcasted_iota(jnp.int32, (rows, 128), 0)
    blocks = [
        jnp.where(iota == index[j : j + 1, :], 1.0, 0.0).astype(BF) for j in range(index.shape[0])
    ]
    return jnp.concatenate(blocks, axis=1)


def silu(u):
    half = 0.5 * u
    return half + half * jnp.tanh(half)


def normed(r, gain, shift):
    centred = r - jnp.mean(r, axis=-1, keepdims=True)
    spread = jnp.mean(centred * centred, axis=-1, keepdims=True)
    return centred * lax.rsqrt(spread + 1e-05) * gain + shift


def tail(pre, out_weight, out_bias, gain, shift):
    hidden = silu(pre).astype(BF)
    return normed(dot(hidden, out_weight[...]) + out_bias[...], gain[...], shift[...])


def fine_kernel(
    live, senders, receivers, before, nodes, after, edges, w1, b1, w2, b2, gain, shift,
    new_edges, sums, by_sender, by_receiver,
):
    width = nodes.shape[1]
    count = nodes.shape[0]
    w_send = w1[width : 2 * width, :]
    by_sender[0:RIM, :] = dot(before[...], w_send).astype(BF)
    by_sender[RIM : RIM + count, :] = dot(nodes[...], w_send).astype(BF)
    by_sender[RIM + count : 2 * RIM + count, :] = dot(after[...], w_send).astype(BF)
    by_receiver[...] = dot(nodes[...], w1[2 * width : 3 * width, :]).astype(BF)
    sums[...] = jnp.zeros_like(sums)
    blocks = TILE // 128

    def step(t, carry):
        base = pl.multiple_of(t * TILE, TILE)
        rows = pl.multiple_of(t * blocks, blocks)
        edge = edges[pl.ds(base, TILE), :]
        from_sender = one_hot_t(count + 2 * RIM, senders[pl.ds(rows, blocks), :])
        from_receiver = one_hot_t(count, receivers[pl.ds(rows, blocks), :])
        pre = dot(edge, w1[0:width, :]) + b1[...]
        pre = pre + dot_t(from_sender, by_sender[...])
        pre = pre + dot_t(from_receiver, by_receiver[...])
        wide = edge.astype(F32)
        updated = wide + tail(pre, w2, b2, gain, shift)
        alive = lax.broadcasted_iota(jnp.int32, updated.shape, 0) + base < live[0]
        new_edges[pl.ds(base, TILE), :] = jnp.where(alive, updated, wide).astype(BF)
        sums[...] += dot(from_receiver, jnp.where(alive, updated, 0.0).astype(BF))
        return carry

    lax.fori_loop(0, edges.shape[0] // TILE, step, 0)


def cross_kernel(
    up_send, up_recv, down_send, down_recv, nodes, coarse, up, down, by_sender, by_receiver, sums,
    w1, b1, w2, b2, gain, shift, v1, c1, v2, c2, node_gain, node_shift,
    new_up, new_down, partial, fine_out,
):
    width = nodes.shape[1]
    count = nodes.shape[0]
    w_edge, w_send, w_recv = (w1[i * width : (i + 1) * width, :] for i in range(3))
    to_coarse = one_hot_t(coarse.shape[0], up_recv[...])
    pre = dot(up[...], w_edge) + b1[...]
    pre = pre + dot_t(one_hot_t(count, up_send[...]), by_sender[RIM : RIM + count, :])
    pre = pre + dot(dot_t(to_coarse, coarse[...]).astype(BF), w_recv)
    updated = (up[...].astype(F32) + tail(pre, w2, b2, gain, shift)).astype(BF)
    new_up[...] = updated
    partial[...] = dot(to_coarse, updated).astype(BF)

    to_fine = one_hot_t(count, down_recv[...])
    pre = dot(down[...], w_edge) + b1[...]
    pre = pre + dot(dot_t(one_hot_t(coarse.shape[0], down_send[...]), coarse[...]).astype(BF), w_send)
    pre = pre + dot_t(to_fine, by_receiver[...])
    updated = (down[...].astype(F32) + tail(pre, w2, b2, gain, shift)).astype(BF)
    new_down[...] = updated
    total = (sums[...] + dot(to_fine, updated)).astype(BF)

    pre = dot(nodes[...], v1[0:width, :]) + c1[...] + dot(total, v1[width : 2 * width, :])
    fine_out[...] = (nodes[...].astype(F32) + tail(pre, v2, c2, node_gain, node_shift)).astype(BF)


def coarse_kernel(parts, coarse, v1, c1, v2, c2, gain, shift, out):
    width = coarse.shape[1]
    total = jnp.sum(parts[...].astype(F32), axis=0).astype(BF)
    pre = dot(coarse[...], v1[0:width, :]) + c1[...] + dot(total, v1[width : 2 * width, :])
    out[...] = (coarse[...].astype(F32) + tail(pre, v2, c2, gain, shift)).astype(BF)


VM = pl.BlockSpec(memory_space=pltpu.VMEM)
SM = pl.BlockSpec(memory_space=pltpu.SMEM)


def call(kernel, outs, args, flops, smem=0):
    shapes = tuple(jax.ShapeDtypeStruct(s, d) for s, d in outs)
    moved = sum(a.size * a.dtype.itemsize for a in args)
    return pl.pallas_call(
        kernel,
        out_shape=shapes,
        in_specs=[SM] * smem + [VM] * (len(args) - smem),
        out_specs=tuple(VM for _ in shapes),
        compiler_params=pltpu.CompilerParams(vmem_limit_bytes=60 * 1024 * 1024),
        cost_estimate=pl.CostEstimate(flops=flops, bytes_accessed=moved, transcendentals=0),
    )(*args)


def swapped(parts, axis):
    return lax.all_to_all(parts, axis, 0, 0, tiled=True)


def body(
    fine_nodes, coarse_nodes, fine_edges, fine_senders, fine_receivers, fine_live,
    up_edges, up_senders, up_receivers, down_edges, down_senders, down_receivers,
    edge_in_weight, edge_in_bias, edge_out_weight, edge_out_bias, edge_gain, edge_shift,
    node_in_weight, node_in_bias, node_out_weight, node_out_bias, node_gain, node_shift,
):
    groups, patches = lax.axis_size("group"), lax.axis_size("patch")
    count, width = fine_nodes.shape
    owned = coarse_nodes.shape[0]
    slots = fine_edges.shape[0]
    lanes = lambda index: index.reshape(-1, 128)
    row = lambda vector: vector.reshape(1, -1)
    edge_net = (
        edge_in_weight, row(edge_in_bias), edge_out_weight, row(edge_out_bias), row(edge_gain),
        row(edge_shift),
    )
    node_net = (
        node_in_weight, row(node_in_bias), node_out_weight, row(node_out_bias), row(node_gain),
        row(node_shift),
    )
    ring = [(i, (i + 1) % patches) for i in range(patches)]
    before = lax.ppermute(fine_nodes[count - RIM :], "patch", ring)
    after = lax.ppermute(fine_nodes[:RIM], "patch", [(j, i) for i, j in ring])
    near = swapped(jnp.broadcast_to(coarse_nodes[None], (patches, owned, width)), "patch")
    near = near.reshape(1, patches * owned, width)
    coarse = swapped(jnp.broadcast_to(near, (groups, patches * owned, width)), "group")
    coarse = coarse.reshape(groups * patches * owned, width)

    new_edges, sums, by_sender, by_receiver = call(
        fine_kernel,
        (
            ((slots, width), BF), ((count, width), F32), ((count + 2 * RIM, width), BF),
            ((count, width), BF),
        ),
        (
            fine_live, lanes(fine_senders), lanes(fine_receivers), before, fine_nodes, after,
            fine_edges, *edge_net,
        ),
        30 * 10**9,
        smem=1,
    )
    new_up, new_down, partial, fine_out = call(
        cross_kernel,
        (
            (up_edges.shape, BF), (down_edges.shape, BF), (coarse.shape, BF), (fine_nodes.shape, BF),
        ),
        (
            lanes(up_senders), lanes(up_receivers), lanes(down_senders), lanes(down_receivers),
            fine_nodes, coarse, up_edges, down_edges, by_sender, by_receiver, sums,
            *edge_net, *node_net,
        ),
        8 * 10**9,
    )
    partial = swapped(partial.reshape(groups, patches, owned, width), "group")
    partial = jnp.sum(partial.astype(F32), axis=0).astype(BF)
    partial = swapped(partial, "patch")
    (coarse_out,) = call(
        coarse_kernel, ((coarse_nodes.shape, BF),), (partial, coarse_nodes, *node_net), 10**8
    )
    return fine_out, coarse_out, new_edges, new_up, new_down


def solution(mesh):
    rows, vector = P(BOTH, None), P(BOTH)
    return jax.shard_map(
        body,
        mesh=mesh,
        in_specs=(rows,) * 3 + (vector,) * 3 + (rows, vector, vector) * 2 + (P(),) * 12,
        out_specs=(rows,) * 5,
        check_vma=False,
    )
```

```python
import functools

import jax
import jax.numpy as jnp
from jax import lax
from jax.experimental import pallas as pl
from jax.experimental.pallas import tpu as pltpu
from jax.sharding import PartitionSpec as P

RIM = 128
BF = jnp.bfloat16
F32 = jnp.float32
TILE = 1024
BOTH = ("group", "patch")
MESH = pl.DeviceIdType.MESH


def dot(a, b):
    return jnp.dot(a, b, preferred_element_type=F32)


def dot_t(a, b):
    return lax.dot_general(a, b, (((0,), (0,)), ((), ())), preferred_element_type=F32)


def one_hot_t(rows, index):
    iota = lax.broadcasted_iota(jnp.int32, (rows, 128), 0)
    blocks = [
        jnp.where(iota == index[j : j + 1, :], 1.0, 0.0).astype(BF) for j in range(index.shape[0])
    ]
    return jnp.concatenate(blocks, axis=1)


def silu(u):
    half = 0.5 * u
    return half + half * jnp.tanh(half)


def normed(r, gain, shift):
    centred = r - jnp.mean(r, axis=-1, keepdims=True)
    spread = jnp.mean(centred * centred, axis=-1, keepdims=True)
    return centred * lax.rsqrt(spread + 1e-05) * gain + shift


def tail(pre, out_weight, out_bias, gain, shift):
    hidden = silu(pre).astype(BF)
    return normed(dot(hidden, out_weight[...]) + out_bias[...], gain[...], shift[...])


def kernel(
    groups, patches,
    live, senders, receivers, up_send, up_recv, down_send, down_recv,
    b1, b2, gain, shift, c1, c2, node_gain, node_shift,
    nodes, coarse, edges, up, down, w1_in, w2_in, v1_in, v2_in,
    fine_out, coarse_out, edges_out, up_out, down_out,
    win, eb, ub, db, w1, w2, v1, v2, by_sender, by_receiver, pre, sums, table, part, beside, half,
    landed, fine_new, coarse_new, up_pre, down_pre,
    load, store, rim_sent, rim_got, spread_sent, spread_got, twin_sent, twin_got, home_sent, home_got,
):
    count, width = nodes.shape
    slots = edges.shape[0]
    owned = coarse.shape[0]
    g, p = lax.axis_index("group"), lax.axis_index("patch")
    core, high = lax.rem(g, 2), g // 2
    chips = groups // 2 * patches
    side = chips * owned
    me = high * patches + p
    twin = (high * 2 + 1 - core, p)
    mine = pl.ds(pl.multiple_of(me * owned, owned), owned)

    def partner(k):
        other = lax.rem(me + k, chips)
        return other, (other // patches * 2 + core, lax.rem(other, patches))

    def each_partner(action):
        def one(k, carry):
            action(*partner(k))
            return carry

        lax.fori_loop(1, chips, one, 0)

    def remote(source, target, sent, got, device):
        return pltpu.make_async_remote_copy(
            source, target, sent, got, device_id=device, device_id_type=MESH
        )

    def settle(ref, sem):
        pltpu.make_async_copy(ref, ref, sem).wait()

    barrier = pltpu.get_barrier_semaphore()

    def greet(other, device):
        pl.semaphore_signal(barrier, inc=1, device_id=device, device_id_type=MESH)

    greet(0, twin)
    each_partner(greet)

    body = pl.ds(RIM, count)
    steps = slots // TILE
    tile = lambda t: pl.ds(pl.multiple_of(t * TILE, TILE), TILE)
    get_nodes = pltpu.make_async_copy(nodes, win.at[body], load.at[0])
    get_w1 = pltpu.make_async_copy(w1_in, w1, load.at[1])
    get_own = pltpu.make_async_copy(coarse, table.at[mine], load.at[2])
    get_w2 = pltpu.make_async_copy(w2_in, w2, load.at[3])
    get_up = pltpu.make_async_copy(up, ub, load.at[4])
    get_down = pltpu.make_async_copy(down, db, load.at[5])
    get_v1 = pltpu.make_async_copy(v1_in, v1, load.at[6])
    get_v2 = pltpu.make_async_copy(v2_in, v2, load.at[7])
    get_edges = lambda t: pltpu.make_async_copy(edges.at[tile(t)], eb.at[tile(t)], load.at[8 + t])
    put_up = pltpu.make_async_copy(ub, up_out, store.at[0])
    put_down = pltpu.make_async_copy(db, down_out, store.at[1])
    put_fine = pltpu.make_async_copy(fine_new, fine_out, store.at[2])
    put_coarse = pltpu.make_async_copy(coarse_new, coarse_out, store.at[3])
    put_edges = lambda t: pltpu.make_async_copy(
        eb.at[tile(t)], edges_out.at[tile(t)], store.at[4 + t]
    )
    get_nodes.start()
    get_w1.start()
    get_own.start()
    get_edges(0).start()
    get_w2.start()
    get_up.start()
    get_down.start()
    for t in range(1, steps):
        get_edges(t).start()
    get_v1.start()
    get_v2.start()

    before = (g, lax.rem(p + patches - 1, patches))
    after = (g, lax.rem(p + 1, patches))
    to_after = remote(
        nodes.at[pl.ds(count - RIM, RIM)], win.at[pl.ds(0, RIM)], rim_sent.at[0], rim_got.at[0], after
    )
    to_before = remote(
        nodes.at[pl.ds(0, RIM)], win.at[pl.ds(RIM + count, RIM)], rim_sent.at[1], rim_got.at[1], before
    )
    same = pl.ds(0, side)
    other_side = pl.ds(side, side)
    table_over = remote(
        table.at[same], table.at[other_side], twin_sent.at[0], twin_got.at[0], twin
    )
    part_over = remote(part.at[other_side], beside, twin_sent.at[1], twin_got.at[1], twin)
    all_but_one = pl.ds(0, side - owned)

    def local_row(index):
        owner, inner = index // (patches * owned), lax.rem(index, patches * owned)
        away = jnp.where(lax.rem(owner, 2) == core, 0, side)
        return owner // 2 * (patches * owned) + inner + away

    get_nodes.wait()
    get_w1.wait()
    w_edge, w_send, w_recv = (w1.at[pl.ds(i * width, width)] for i in range(3))
    by_sender[RIM : RIM + count, :] = dot(win[RIM : RIM + count, :], w_send[...]).astype(BF)
    by_receiver[...] = dot(win[RIM : RIM + count, :], w_recv[...]).astype(BF)
    sums[...] = jnp.zeros_like(sums)

    pl.semaphore_wait(barrier, chips)
    to_after.start()
    to_before.start()

    def spread(other, device):
        remote(coarse, table.at[mine], spread_sent, spread_got, device).start()

    each_partner(spread)
    blocks = TILE // 128

    def up_stage():
        settle(table.at[all_but_one], spread_got)
        get_own.wait()
        table_over.start()
        get_up.wait()
        get_down.wait()
        up_pre[...] = (
            dot(ub[...], w_edge[...])
            + b1[...]
            + dot_t(one_hot_t(count, up_send[...]), by_sender[RIM : RIM + count, :])
        )
        down_pre[...] = (
            dot(db[...], w_edge[...])
            + b1[...]
            + dot_t(one_hot_t(count, down_recv[...]), by_receiver[...])
        )
        table_over.wait_recv()
        to_coarse = one_hot_t(2 * side, local_row(up_recv[...]))
        picked = dot_t(to_coarse, table[...]).astype(BF)
        new = tail(up_pre[...] + dot(picked, w_recv[...]), w2, b2, gain, shift)
        new = (ub[...].astype(F32) + new).astype(BF)
        ub[...] = new
        put_up.start()
        part[...] = dot(to_coarse, new).astype(BF)
        part_over.start()

    def home_stage():
        part_over.wait_recv()
        half[...] = (part[0:side, :].astype(F32) + beside[...].astype(F32)).astype(BF)
        landed[mine, :] = half[mine, :]

        def home(other, device):
            rows = pl.ds(pl.multiple_of(other * owned, owned), owned)
            remote(half.at[rows], landed.at[mine], home_sent, home_got, device).start()

        each_partner(home)

    def step(t, carry):
        base = pl.multiple_of(t * TILE, TILE)
        rows = pl.ds(pl.multiple_of(t * blocks, blocks), blocks)
        pl.when(t == steps // 2)(up_stage)
        pl.when(t == steps // 2 + 1)(home_stage)
        get_edges(t).wait()
        send_row = senders[rows, :]
        from_receiver = one_hot_t(count, receivers[rows, :])
        pre[...] = (
            dot(eb[tile(t), :], w_edge[...])
            + b1[...]
            + dot_t(one_hot_t(count, send_row - RIM), by_sender[RIM : RIM + count, :])
            + dot_t(from_receiver, by_receiver[...])
        )

        @pl.when(t == 0)
        def _():
            to_after.wait_recv()
            to_before.wait_recv()
            by_sender[0:RIM, :] = dot(win[0:RIM, :], w_send[...]).astype(BF)
            by_sender[RIM + count :, :] = dot(win[RIM + count :, :], w_send[...]).astype(BF)

        full = (
            pre[...]
            + dot_t(one_hot_t(RIM, send_row), by_sender[0:RIM, :])
            + dot_t(one_hot_t(RIM, send_row - (RIM + count)), by_sender[RIM + count :, :])
        )
        wide = eb[tile(t), :].astype(F32)
        updated = wide + tail(full, w2, b2, gain, shift)
        alive = lax.broadcasted_iota(jnp.int32, updated.shape, 0) + base < live[0]
        sums[...] += dot(
            one_hot_t(count, receivers[rows, :]), jnp.where(alive, updated, 0.0).astype(BF)
        )
        eb[tile(t), :] = jnp.where(alive, updated, wide).astype(BF)
        put_edges(t).start()
        return carry

    get_w2.wait()
    lax.fori_loop(0, steps, step, 0)

    picked = dot_t(one_hot_t(2 * side, local_row(down_send[...])), table[...]).astype(BF)
    new = tail(down_pre[...] + dot(picked, w_send[...]), w2, b2, gain, shift)
    new = (db[...].astype(F32) + new).astype(BF)
    db[...] = new
    put_down.start()
    total = (sums[...] + dot(one_hot_t(count, down_recv[...]), new)).astype(BF)
    get_v1.wait()
    get_v2.wait()

    def node_net(old, summed):
        inner = dot(old, v1[0:width, :]) + c1[...] + dot(summed, v1[width : 2 * width, :])
        return (old.astype(F32) + tail(inner, v2, c2, node_gain, node_shift)).astype(BF)

    fine_new[...] = node_net(win[RIM : RIM + count, :], total)
    put_fine.start()

    settle(landed.at[all_but_one], home_got)
    arrived = jnp.sum(landed[...].astype(F32).reshape(chips, owned, width), axis=0).astype(BF)
    coarse_new[...] = node_net(table[mine, :], arrived)
    put_coarse.start()

    to_after.wait_send()
    to_before.wait_send()
    settle(table.at[all_but_one], spread_sent)
    settle(half.at[all_but_one], home_sent)
    table_over.wait_send()
    part_over.wait_send()
    for copy in (put_up, put_down, put_fine, put_coarse):
        copy.wait()
    for t in range(steps):
        put_edges(t).wait()


def body(
    fine_nodes, coarse_nodes, fine_edges, fine_senders, fine_receivers, fine_live,
    up_edges, up_senders, up_receivers, down_edges, down_senders, down_receivers,
    edge_in_weight, edge_in_bias, edge_out_weight, edge_out_bias, edge_gain, edge_shift,
    node_in_weight, node_in_bias, node_out_weight, node_out_bias, node_gain, node_shift,
):
    groups, patches = lax.axis_size("group"), lax.axis_size("patch")
    count, width = fine_nodes.shape
    owned = coarse_nodes.shape[0]
    slots = fine_edges.shape[0]
    crossing = up_edges.shape[0]
    everywhere = groups * patches * owned
    side = everywhere // 2
    steps = slots // TILE
    lanes = lambda index: index.reshape(-1, 128)
    row = lambda vector: vector.reshape(1, -1)
    vm = pl.BlockSpec(memory_space=pltpu.VMEM)
    anywhere = pl.BlockSpec(memory_space=pl.ANY)
    outs = (fine_nodes, coarse_nodes, fine_edges, up_edges, down_edges)
    rows = lambda n, dtype=BF: pltpu.VMEM((n, width), dtype)
    dma = pltpu.SemaphoreType.DMA
    return pl.pallas_call(
        functools.partial(kernel, groups, patches),
        out_shape=tuple(jax.ShapeDtypeStruct(a.shape, a.dtype) for a in outs),
        in_specs=[pl.BlockSpec(memory_space=pltpu.SMEM)] + [vm] * 14 + [anywhere] * 9,
        out_specs=(anywhere,) * 5,
        scratch_shapes=[
            rows(count + 2 * RIM), rows(slots), rows(crossing), rows(crossing),
            rows(3 * width), rows(width), rows(2 * width), rows(width),
            rows(count + 2 * RIM), rows(count), rows(TILE, F32), rows(count, F32),
            rows(everywhere), rows(everywhere), rows(side), rows(side), rows(side),
            rows(count), rows(owned), rows(crossing, F32), rows(crossing, F32),
            dma((8 + steps,)), dma((4 + steps,)), dma((2,)), dma((2,)),
            dma(()), dma(()), dma((2,)), dma((2,)), dma(()), dma(()),
        ],
        compiler_params=pltpu.CompilerParams(
            vmem_limit_bytes=62 * 1024 * 1024, collective_id=0, has_side_effects=True
        ),
    )(
        fine_live, lanes(fine_senders), lanes(fine_receivers), lanes(up_senders),
        lanes(up_receivers), lanes(down_senders), lanes(down_receivers),
        row(edge_in_bias), row(edge_out_bias), row(edge_gain), row(edge_shift),
        row(node_in_bias), row(node_out_bias), row(node_gain), row(node_shift),
        fine_nodes, coarse_nodes, fine_edges, up_edges, down_edges,
        edge_in_weight, edge_out_weight, node_in_weight, node_out_weight,
    )


def solution(mesh):
    rows, vector = P(BOTH, None), P(BOTH)
    return jax.shard_map(
        body,
        mesh=mesh,
        in_specs=(rows,) * 3 + (vector,) * 3 + (rows, vector, vector) * 2 + (P(),) * 12,
        out_specs=(rows,) * 5,
        check_vma=False,
    )
```

```python
import functools

import jax
import jax.numpy as jnp
from jax import lax
from jax.experimental import pallas as pl
from jax.experimental.pallas import tpu as pltpu
from jax.sharding import PartitionSpec as P

RIM = 128
BF = jnp.bfloat16
F32 = jnp.float32
TILE = 1024
BOTH = ("group", "patch")
MESH = pl.DeviceIdType.MESH


def dot(a, b):
    return jnp.dot(a, b, preferred_element_type=F32)


def dot_t(a, b):
    return lax.dot_general(a, b, (((0,), (0,)), ((), ())), preferred_element_type=F32)


def one_hot_t(rows, index):
    iota = lax.broadcasted_iota(jnp.int32, (rows, 128), 0)
    blocks = [
        jnp.where(iota == index[j : j + 1, :], 1.0, 0.0).astype(BF) for j in range(index.shape[0])
    ]
    return jnp.concatenate(blocks, axis=1)


def silu(u):
    half = 0.5 * u
    return half + half * jnp.tanh(half)


def normed(r, gain, shift):
    centred = r - jnp.mean(r, axis=-1, keepdims=True)
    spread = jnp.mean(centred * centred, axis=-1, keepdims=True)
    return centred * lax.rsqrt(spread + 1e-05) * gain + shift


def tail(pre, out_weight, out_bias, gain, shift):
    hidden = silu(pre).astype(BF)
    return normed(dot(hidden, out_weight[...]) + out_bias[...], gain[...], shift[...])


def kernel(
    groups, patches,
    live, senders_in, receivers_in, up_send_in, up_recv_in, down_send_in, down_recv_in,
    b1_in, b2_in, gain_in, shift_in, c1_in, c2_in, node_gain_in, node_shift_in,
    nodes, coarse, edges, up, down, w1_in, w2_in, v1_in, v2_in,
    fine_new, coarse_new, eb, ub, db,
    win, w1, w2, v1, v2, by_sender, by_receiver, pre, sums, table, part, beside, half,
    landed, up_pre, down_pre,
    senders, receivers, up_send, up_recv, down_send, down_recv,
    b1, b2, gain, shift, c1, c2, node_gain, node_shift,
    load, few, rim_sent, rim_got, spread_sent, spread_got, twin_sent, twin_got, home_sent, home_got,
):
    count, width = nodes.shape
    slots = edges.shape[0]
    owned = coarse.shape[0]
    g, p = lax.axis_index("group"), lax.axis_index("patch")
    core, high = lax.rem(g, 2), g // 2
    chips = groups // 2 * patches
    side = chips * owned
    me = high * patches + p
    twin = (high * 2 + 1 - core, p)
    mine = pl.ds(pl.multiple_of(me * owned, owned), owned)

    def each_partner(action):
        def one(k, carry):
            other = lax.rem(me + k, chips)
            action(other, (other // patches * 2 + core, lax.rem(other, patches)))
            return carry

        lax.fori_loop(1, chips, one, 0)

    def remote(source, target, sent, got, device):
        return pltpu.make_async_remote_copy(
            source, target, sent, got, device_id=device, device_id_type=MESH
        )

    def settle(ref, sem):
        pltpu.make_async_copy(ref, ref, sem).wait()

    barrier = pltpu.get_barrier_semaphore()

    def greet(other, device):
        pl.semaphore_signal(barrier, inc=1, device_id=device, device_id_type=MESH)

    greet(0, twin)
    each_partner(greet)

    steps = slots // TILE
    early = steps - 1
    tile = lambda t: pl.ds(pl.multiple_of(t * TILE, TILE), TILE)
    own_rows = slice(RIM, RIM + count)
    get_nodes = pltpu.make_async_copy(nodes, win.at[pl.ds(RIM, count)], load.at[0])
    get_w1 = pltpu.make_async_copy(w1_in, w1, load.at[1])
    get_own = pltpu.make_async_copy(coarse, table.at[mine], load.at[2])
    get_w2 = pltpu.make_async_copy(w2_in, w2, load.at[3])
    get_up = pltpu.make_async_copy(up, ub, load.at[4])
    get_down = pltpu.make_async_copy(down, db, load.at[5])
    get_v1 = pltpu.make_async_copy(v1_in, v1, load.at[6])
    get_v2 = pltpu.make_async_copy(v2_in, v2, load.at[7])
    get_edges = lambda t: pltpu.make_async_copy(edges.at[tile(t)], eb.at[tile(t)], load.at[8 + t])
    small = (
        (senders_in, senders), (receivers_in, receivers), (up_send_in, up_send),
        (up_recv_in, up_recv), (down_send_in, down_send), (down_recv_in, down_recv),
        (b1_in, b1), (b2_in, b2), (gain_in, gain), (shift_in, shift), (c1_in, c1), (c2_in, c2),
        (node_gain_in, node_gain), (node_shift_in, node_shift),
    )
    small = [pltpu.make_async_copy(a, b, few.at[i]) for i, (a, b) in enumerate(small)]
    get_nodes.start()
    get_w1.start()
    for copy in small:
        copy.start()
    get_own.start()
    get_up.start()
    get_down.start()
    for t in range(early):
        get_edges(t).start()
    get_w2.start()
    get_edges(early).start()
    get_v1.start()
    get_v2.start()

    before = (g, lax.rem(p + patches - 1, patches))
    after = (g, lax.rem(p + 1, patches))
    to_after = remote(
        nodes.at[pl.ds(count - RIM, RIM)], win.at[pl.ds(0, RIM)], rim_sent.at[0], rim_got.at[0], after
    )
    to_before = remote(
        nodes.at[pl.ds(0, RIM)], win.at[pl.ds(RIM + count, RIM)], rim_sent.at[1], rim_got.at[1], before
    )
    same = pl.ds(0, side)
    other_side = pl.ds(side, side)
    table_over = remote(
        table.at[same], table.at[other_side], twin_sent.at[0], twin_got.at[0], twin
    )
    part_over = remote(part.at[other_side], beside, twin_sent.at[1], twin_got.at[1], twin)
    all_but_one = pl.ds(0, side - owned)

    def spread(other, device):
        remote(coarse, table.at[mine], spread_sent, spread_got, device).start()

    with jax.named_scope("wait_bar"):
        pl.semaphore_wait(barrier, chips)
    each_partner(spread)
    to_after.start()
    to_before.start()

    def local_row(index):
        owner, inner = index // (patches * owned), lax.rem(index, patches * owned)
        away = jnp.where(lax.rem(owner, 2) == core, 0, side)
        return owner // 2 * (patches * owned) + inner + away

    with jax.named_scope("wait_load"):
        get_nodes.wait()
        get_w1.wait()
    w_edge, w_send, w_recv = (w1.at[pl.ds(i * width, width)] for i in range(3))
    by_sender[own_rows, :] = dot(win[own_rows, :], w_send[...]).astype(BF)
    by_receiver[...] = dot(win[own_rows, :], w_recv[...]).astype(BF)
    sums[...] = jnp.zeros_like(sums)
    for copy in small:
        copy.wait()
    get_up.wait()
    up_pre[...] = (
        dot(ub[...], w_edge[...])
        + b1[...]
        + dot_t(one_hot_t(count, up_send[...]), by_sender[own_rows, :])
    )
    get_down.wait()
    down_pre[...] = (
        dot(db[...], w_edge[...])
        + b1[...]
        + dot_t(one_hot_t(count, down_recv[...]), by_receiver[...])
    )
    blocks = TILE // 128
    index_rows = lambda t: pl.ds(pl.multiple_of(t * blocks, blocks), blocks)

    def main(t):
        get_edges(t).wait()
        pre[tile(t), :] = (
            dot(eb[tile(t), :], w_edge[...])
            + b1[...]
            + dot_t(one_hot_t(count, senders[index_rows(t), :] - RIM), by_sender[own_rows, :])
            + dot_t(one_hot_t(count, receivers[index_rows(t), :]), by_receiver[...])
        )

    def early_step(t, carry):
        main(t)
        return carry

    lax.fori_loop(0, early, early_step, 0)
    get_w2.wait()
    with jax.named_scope("wait_rim"):
        to_after.wait_recv()
        to_before.wait_recv()
    with jax.named_scope("wait_spread"):
        settle(table.at[all_but_one], spread_got)
    get_own.wait()
    table_over.start()
    by_sender[0:RIM, :] = dot(win[0:RIM, :], w_send[...]).astype(BF)
    by_sender[RIM + count :, :] = dot(win[RIM + count :, :], w_send[...]).astype(BF)

    @jax.named_scope("up")
    def up_stage():
        with jax.named_scope("wait_twin"):
            table_over.wait_recv()
        to_coarse = one_hot_t(2 * side, local_row(up_recv[...]))
        picked = dot_t(to_coarse, table[...]).astype(BF)
        new = tail(up_pre[...] + dot(picked, w_recv[...]), w2, b2, gain, shift)
        new = (ub[...].astype(F32) + new).astype(BF)
        ub[...] = new
        part[...] = dot(to_coarse, new).astype(BF)
        part_over.start()

    @jax.named_scope("home")
    def home_stage():
        with jax.named_scope("wait_part"):
            part_over.wait_recv()
        half[...] = (part[0:side, :].astype(F32) + beside[...].astype(F32)).astype(BF)
        landed[mine, :] = half[mine, :]

        def home(other, device):
            rows = pl.ds(pl.multiple_of(other * owned, owned), owned)
            remote(half.at[rows], landed.at[mine], home_sent, home_got, device).start()

        each_partner(home)

    def step(t, carry):
        base = pl.multiple_of(t * TILE, TILE)
        pl.when(t == 1)(up_stage)
        pl.when(t == 2)(home_stage)
        pl.when(t == early)(lambda: main(t))
        send_row = senders[index_rows(t), :]
        full = (
            pre[tile(t), :]
            + dot_t(one_hot_t(RIM, send_row), by_sender[0:RIM, :])
            + dot_t(one_hot_t(RIM, send_row - (RIM + count)), by_sender[RIM + count :, :])
        )
        wide = eb[tile(t), :].astype(F32)
        updated = wide + tail(full, w2, b2, gain, shift)
        alive = lax.broadcasted_iota(jnp.int32, updated.shape, 0) + base < live[0]
        sums[...] += dot(
            one_hot_t(count, receivers[index_rows(t), :]), jnp.where(alive, updated, 0.0).astype(BF)
        )
        eb[tile(t), :] = jnp.where(alive, updated, wide).astype(BF)
        return carry

    lax.fori_loop(0, steps, step, 0)

    with jax.named_scope("down"):
        picked = dot_t(one_hot_t(2 * side, local_row(down_send[...])), table[...]).astype(BF)
        new = tail(down_pre[...] + dot(picked, w_send[...]), w2, b2, gain, shift)
        new = (db[...].astype(F32) + new).astype(BF)
        db[...] = new
        total = (sums[...] + dot(one_hot_t(count, down_recv[...]), new)).astype(BF)
    get_v1.wait()
    get_v2.wait()

    def node_net(old, summed):
        inner = dot(old, v1[0:width, :]) + c1[...] + dot(summed, v1[width : 2 * width, :])
        return (old.astype(F32) + tail(inner, v2, c2, node_gain, node_shift)).astype(BF)

    with jax.named_scope("node"):
        fine_new[...] = node_net(win[own_rows, :], total)

    with jax.named_scope("wait_home"):
        settle(landed.at[all_but_one], home_got)
    with jax.named_scope("ends"):
        arrived = jnp.sum(landed[...].astype(F32).reshape(chips, owned, width), axis=0).astype(BF)
        coarse_new[...] = node_net(table[mine, :], arrived)
        to_after.wait_send()
        to_before.wait_send()
        settle(table.at[all_but_one], spread_sent)
        settle(half.at[all_but_one], home_sent)
        table_over.wait_send()
        part_over.wait_send()


def writer(fine, coarse, edges, up, down, *outs_and_sem):
    *outs, sem = outs_and_sem
    copies = []
    for source, target in zip((edges, fine, up, down, coarse), (outs[2], outs[0], *outs[3:], outs[1])):
        size = min(source.shape[0], 512)
        for at in range(0, source.shape[0], size):
            rows = pl.ds(at, size)
            copies.append(pltpu.make_async_copy(source.at[rows], target.at[rows], sem.at[len(copies)]))
    for copy in copies:
        copy.start()
    for copy in copies:
        copy.wait()


def body(
    fine_nodes, coarse_nodes, fine_edges, fine_senders, fine_receivers, fine_live,
    up_edges, up_senders, up_receivers, down_edges, down_senders, down_receivers,
    edge_in_weight, edge_in_bias, edge_out_weight, edge_out_bias, edge_gain, edge_shift,
    node_in_weight, node_in_bias, node_out_weight, node_out_bias, node_gain, node_shift,
):
    groups, patches = lax.axis_size("group"), lax.axis_size("patch")
    count, width = fine_nodes.shape
    owned = coarse_nodes.shape[0]
    slots = fine_edges.shape[0]
    crossing = up_edges.shape[0]
    everywhere = groups * patches * owned
    side = everywhere // 2
    steps = slots // TILE
    lanes = lambda index: index.reshape(-1, 128)
    row = lambda vector: vector.reshape(1, -1)
    vm = pl.BlockSpec(memory_space=pltpu.VMEM)
    anywhere = pl.BlockSpec(memory_space=pl.ANY)
    outs = (fine_nodes, coarse_nodes, fine_edges, up_edges, down_edges)
    rows = lambda n, dtype=BF: pltpu.VMEM((n, width), dtype)
    dma = pltpu.SemaphoreType.DMA
    indices = tuple(
        lanes(a)
        for a in (fine_senders, fine_receivers, up_senders, up_receivers, down_senders, down_receivers)
    )
    vectors = tuple(
        row(a)
        for a in (
            edge_in_bias, edge_out_bias, edge_gain, edge_shift,
            node_in_bias, node_out_bias, node_gain, node_shift,
        )
    )
    results = pl.pallas_call(
        functools.partial(kernel, groups, patches),
        out_shape=tuple(pltpu.VMEM(a.shape, a.dtype) for a in outs),
        in_specs=[pl.BlockSpec(memory_space=pltpu.SMEM)] + [anywhere] * 23,
        out_specs=(vm,) * 5,
        scratch_shapes=[
            rows(count + 2 * RIM),
            rows(3 * width), rows(width), rows(2 * width), rows(width),
            rows(count + 2 * RIM), rows(count), rows(slots, F32), rows(count, F32),
            rows(everywhere), rows(everywhere), rows(side), rows(side), rows(side),
            rows(crossing, F32), rows(crossing, F32),
            *(pltpu.VMEM(a.shape, a.dtype) for a in indices + vectors),
            dma((8 + steps,)), dma((len(indices + vectors),)), dma((2,)), dma((2,)),
            dma(()), dma(()), dma((2,)), dma((2,)), dma(()), dma(()),
        ],
        compiler_params=pltpu.CompilerParams(
            vmem_limit_bytes=50 * 1024 * 1024, collective_id=0, has_side_effects=True
        ),
    )(
        fine_live, *indices, *vectors,
        fine_nodes, coarse_nodes, fine_edges, up_edges, down_edges,
        edge_in_weight, edge_out_weight, node_in_weight, node_out_weight,
    )
    return pl.pallas_call(
        writer,
        out_shape=tuple(jax.ShapeDtypeStruct(a.shape, a.dtype) for a in outs),
        in_specs=[vm] * 5,
        out_specs=(anywhere,) * 5,
        scratch_shapes=[dma((slots // 512 + count // 512 + 3,))],
        compiler_params=pltpu.CompilerParams(vmem_limit_bytes=2**20),
    )(*results)


def solution(mesh):
    rows, vector = P(BOTH, None), P(BOTH)
    return jax.shard_map(
        body,
        mesh=mesh,
        in_specs=(rows,) * 3 + (vector,) * 3 + (rows, vector, vector) * 2 + (P(),) * 12,
        out_specs=(rows,) * 5,
        check_vma=False,
    )
```

```python
import functools

import jax
import jax.numpy as jnp
from jax import lax
from jax.experimental import pallas as pl
from jax.experimental.pallas import tpu as pltpu
from jax.sharding import PartitionSpec as P

RIM = 128
BF = jnp.bfloat16
F32 = jnp.float32
TILE = 1024
BOTH = ("group", "patch")
MESH = pl.DeviceIdType.MESH


def dot(a, b):
    return jnp.dot(a, b, preferred_element_type=F32)


def dot_t(a, b):
    return lax.dot_general(a, b, (((0,), (0,)), ((), ())), preferred_element_type=F32)


def one_hot_t(rows, index):
    iota = lax.broadcasted_iota(jnp.int32, (rows, 128), 0)
    blocks = [
        jnp.where(iota == index[j : j + 1, :], 1.0, 0.0).astype(BF) for j in range(index.shape[0])
    ]
    return jnp.concatenate(blocks, axis=1)


def silu(u):
    half = 0.5 * u
    return half + half * jnp.tanh(half)


def normed(r, gain, shift):
    centred = r - jnp.mean(r, axis=-1, keepdims=True)
    spread = jnp.mean(centred * centred, axis=-1, keepdims=True)
    return centred * lax.rsqrt(spread + 1e-05) * gain + shift


def tail(pre, out_weight, out_bias, gain, shift):
    hidden = silu(pre).astype(BF)
    return normed(dot(hidden, out_weight[...]) + out_bias[...], gain[...], shift[...])


def kernel(
    groups, patches,
    live, senders_in, receivers_in, up_send_in, up_recv_in, down_send_in, down_recv_in,
    b1_in, b2_in, gain_in, shift_in, c1_in, c2_in, node_gain_in, node_shift_in,
    nodes, coarse, edges, up, down, w1_in, w2_in, v1_in, v2_in,
    fine_new, coarse_new, eb, ub, db,
    win, w1, w2, v1, v2, by_sender, by_receiver, pre, sums, table, part, beside, half,
    landed, up_pre, down_pre,
    senders, receivers, up_send, up_recv, down_send, down_recv,
    b1, b2, gain, shift, c1, c2, node_gain, node_shift,
    load, few, rim_sent, rim_got, spread_sent, spread_got, twin_sent, twin_got, home_sent, home_got,
):
    count, width = nodes.shape
    slots = edges.shape[0]
    owned = coarse.shape[0]
    g, p = lax.axis_index("group"), lax.axis_index("patch")
    core, high = lax.rem(g, 2), g // 2
    chips = groups // 2 * patches
    side = chips * owned
    me = high * patches + p
    planes = 4
    plane = chips // planes
    mine_y, mine_xz = me // plane, lax.rem(me, plane)
    band = plane * owned
    twin = (high * 2 + 1 - core, p)
    mine = pl.ds(pl.multiple_of(me * owned, owned), owned)

    def in_plane(ahead, action):
        y = lax.rem(mine_y + ahead, planes)

        def one(k, carry):
            other = y * plane + lax.rem(mine_xz + k, plane)
            action(other, (other // patches * 2 + core, lax.rem(other, patches)))
            return carry

        lax.fori_loop(0 if ahead else 1, plane, one, 0)

    def ahead_rows(ahead, start=0):
        y = lax.rem(mine_y + ahead + planes, planes)
        return pl.ds(pl.multiple_of(y * band + start, band), band)

    def remote(source, target, sent, got, device):
        return pltpu.make_async_remote_copy(
            source, target, sent, got, device_id=device, device_id_type=MESH
        )

    def settle(ref, sem):
        pltpu.make_async_copy(ref, ref, sem).wait()

    barrier = pltpu.get_barrier_semaphore()

    def greet(other, device):
        pl.semaphore_signal(barrier, inc=1, device_id=device, device_id_type=MESH)

    greet(0, twin)
    for ahead in range(planes):
        in_plane(ahead, greet)

    steps = slots // TILE
    early = steps - 1
    tile = lambda t: pl.ds(pl.multiple_of(t * TILE, TILE), TILE)
    own_rows = slice(RIM, RIM + count)
    get_nodes = pltpu.make_async_copy(nodes, win.at[pl.ds(RIM, count)], load.at[0])
    get_w1 = pltpu.make_async_copy(w1_in, w1, load.at[1])
    get_own = pltpu.make_async_copy(coarse, table.at[mine], load.at[2])
    get_w2 = pltpu.make_async_copy(w2_in, w2, load.at[3])
    get_up = pltpu.make_async_copy(up, ub, load.at[4])
    get_down = pltpu.make_async_copy(down, db, load.at[5])
    get_v1 = pltpu.make_async_copy(v1_in, v1, load.at[6])
    get_v2 = pltpu.make_async_copy(v2_in, v2, load.at[7])
    get_edges = lambda t: pltpu.make_async_copy(edges.at[tile(t)], eb.at[tile(t)], load.at[8 + t])
    small = (
        (senders_in, senders), (receivers_in, receivers), (up_send_in, up_send),
        (up_recv_in, up_recv), (down_send_in, down_send), (down_recv_in, down_recv),
        (b1_in, b1), (b2_in, b2), (gain_in, gain), (shift_in, shift), (c1_in, c1), (c2_in, c2),
        (node_gain_in, node_gain), (node_shift_in, node_shift),
    )
    small = [pltpu.make_async_copy(a, b, few.at[i]) for i, (a, b) in enumerate(small)]
    get_nodes.start()
    get_w1.start()
    get_own.start()

    before = (g, lax.rem(p + patches - 1, patches))
    after = (g, lax.rem(p + 1, patches))
    to_after = remote(
        nodes.at[pl.ds(count - RIM, RIM)], win.at[pl.ds(0, RIM)], rim_sent.at[0], rim_got.at[0], after
    )
    to_before = remote(
        nodes.at[pl.ds(0, RIM)], win.at[pl.ds(RIM + count, RIM)], rim_sent.at[1], rim_got.at[1], before
    )
    same = pl.ds(0, side)
    other_side = pl.ds(side, side)
    table_over = lambda ahead: remote(
        table.at[ahead_rows(-ahead)],
        table.at[ahead_rows(-ahead, side)],
        twin_sent.at[ahead],
        twin_got.at[ahead],
        twin,
    )
    part_over = lambda ahead: remote(
        part.at[ahead_rows(ahead, side)],
        beside.at[ahead_rows(ahead)],
        twin_sent.at[planes + ahead],
        twin_got.at[planes + ahead],
        twin,
    )
    all_but_one = pl.ds(0, side - owned)
    arriving = lambda ahead: pl.ds(0, band if ahead else band - owned)

    def spread(ahead):
        def send(other, device):
            remote(coarse, table.at[mine], spread_sent, spread_got.at[ahead], device).start()

        in_plane(ahead, send)

    with jax.named_scope("wait_bar"):
        pl.semaphore_wait(barrier, chips)
    for ahead in range(planes):
        spread(ahead)
    get_up.start()
    for copy in small:
        copy.start()
    get_down.start()
    for t in range(early):
        get_edges(t).start()
    get_w2.start()
    get_edges(early).start()
    get_v1.start()
    get_v2.start()

    def local_row(index):
        owner, inner = index // (patches * owned), lax.rem(index, patches * owned)
        away = jnp.where(lax.rem(owner, 2) == core, 0, side)
        return owner // 2 * (patches * owned) + inner + away

    with jax.named_scope("wait_load"):
        get_nodes.wait()
        get_w1.wait()
    w_edge, w_send, w_recv = (w1.at[pl.ds(i * width, width)] for i in range(3))
    by_sender[own_rows, :] = dot(win[own_rows, :], w_send[...]).astype(BF)
    by_receiver[...] = dot(win[own_rows, :], w_recv[...]).astype(BF)
    for copy in small:
        copy.wait()
    get_up.wait()
    up_pre[...] = (
        dot(ub[...], w_edge[...])
        + b1[...]
        + dot_t(one_hot_t(count, up_send[...]), by_sender[own_rows, :])
    )
    get_down.wait()
    down_pre[...] = (
        dot(db[...], w_edge[...])
        + b1[...]
        + dot_t(one_hot_t(count, down_recv[...]), by_receiver[...])
    )
    blocks = TILE // 128
    index_rows = lambda t: pl.ds(pl.multiple_of(t * blocks, blocks), blocks)

    def main(t):
        get_edges(t).wait()
        pre[tile(t), :] = (
            dot(eb[tile(t), :], w_edge[...])
            + b1[...]
            + dot_t(one_hot_t(count, senders[index_rows(t), :] - RIM), by_sender[own_rows, :])
            + dot_t(one_hot_t(count, receivers[index_rows(t), :]), by_receiver[...])
        )

    def early_step(t, carry):
        main(t)
        return carry

    lax.fori_loop(0, early, early_step, 0)
    get_own.wait()
    for ahead in range(planes):
        with jax.named_scope("wait_spread"):
            settle(table.at[arriving(ahead)], spread_got.at[ahead])
        table_over(ahead).start()
    to_after.start()
    to_before.start()
    main(early)
    get_w2.wait()

    with jax.named_scope("up"):
        with jax.named_scope("wait_twin"):
            for ahead in range(planes):
                table_over(ahead).wait_recv()
        to_coarse = one_hot_t(2 * side, local_row(up_recv[...]))
        picked = dot_t(to_coarse, table[...]).astype(BF)
        new = tail(up_pre[...] + dot(picked, w_recv[...]), w2, b2, gain, shift)
        new = (ub[...].astype(F32) + new).astype(BF)
        ub[...] = new
        part[...] = dot(to_coarse, new).astype(BF)
        for ahead in range(planes):
            part_over(ahead).start()

    with jax.named_scope("down"):
        picked = dot_t(one_hot_t(2 * side, local_row(down_send[...])), table[...]).astype(BF)
        new = tail(down_pre[...] + dot(picked, w_send[...]), w2, b2, gain, shift)
        new = (db[...].astype(F32) + new).astype(BF)
        db[...] = new
        sums[...] = dot(one_hot_t(count, down_recv[...]), new)

    with jax.named_scope("home"):
        for ahead in range(planes):
            part_over(ahead).wait_recv()
            rows = ahead_rows(ahead)
            half[rows, :] = (part[rows, :].astype(F32) + beside[rows, :].astype(F32)).astype(BF)

            def home(other, device):
                block = pl.ds(pl.multiple_of(other * owned, owned), owned)
                remote(half.at[block], landed.at[mine], home_sent, home_got, device).start()

            in_plane(ahead, home)
        landed[mine, :] = half[mine, :]

    with jax.named_scope("wait_rim"):
        to_after.wait_recv()
        to_before.wait_recv()
    by_sender[0:RIM, :] = dot(win[0:RIM, :], w_send[...]).astype(BF)
    by_sender[RIM + count :, :] = dot(win[RIM + count :, :], w_send[...]).astype(BF)

    def step(t, carry):
        base = pl.multiple_of(t * TILE, TILE)
        send_row = senders[index_rows(t), :]
        full = (
            pre[tile(t), :]
            + dot_t(one_hot_t(RIM, send_row), by_sender[0:RIM, :])
            + dot_t(one_hot_t(RIM, send_row - (RIM + count)), by_sender[RIM + count :, :])
        )
        wide = eb[tile(t), :].astype(F32)
        updated = wide + tail(full, w2, b2, gain, shift)
        alive = lax.broadcasted_iota(jnp.int32, updated.shape, 0) + base < live[0]
        sums[...] += dot(
            one_hot_t(count, receivers[index_rows(t), :]), jnp.where(alive, updated, 0.0).astype(BF)
        )
        eb[tile(t), :] = jnp.where(alive, updated, wide).astype(BF)
        return carry

    with jax.named_scope("tails"):
        lax.fori_loop(0, steps, step, 0)
    get_v1.wait()
    get_v2.wait()

    def node_net(old, summed):
        inner = dot(old, v1[0:width, :]) + c1[...] + dot(summed, v1[width : 2 * width, :])
        return (old.astype(F32) + tail(inner, v2, c2, node_gain, node_shift)).astype(BF)

    with jax.named_scope("node"):
        fine_new[...] = node_net(win[own_rows, :], sums[...].astype(BF))

    with jax.named_scope("wait_home"):
        settle(landed.at[all_but_one], home_got)
    with jax.named_scope("ends"):
        arrived = jnp.sum(landed[...].astype(F32).reshape(chips, owned, width), axis=0).astype(BF)
        coarse_new[...] = node_net(table[mine, :], arrived)
        to_after.wait_send()
        to_before.wait_send()
        settle(table.at[all_but_one], spread_sent)
        settle(half.at[all_but_one], home_sent)
        for ahead in range(planes):
            table_over(ahead).wait_send()
            part_over(ahead).wait_send()


def writer(fine, coarse, edges, up, down, *outs_and_sem):
    *outs, sem = outs_and_sem
    copies = []
    for source, target in zip((edges, fine, up, down, coarse), (outs[2], outs[0], *outs[3:], outs[1])):
        size = min(source.shape[0], 512)
        for at in range(0, source.shape[0], size):
            rows = pl.ds(at, size)
            copies.append(pltpu.make_async_copy(source.at[rows], target.at[rows], sem.at[len(copies)]))
    for copy in copies:
        copy.start()
    for copy in copies:
        copy.wait()


def body(
    fine_nodes, coarse_nodes, fine_edges, fine_senders, fine_receivers, fine_live,
    up_edges, up_senders, up_receivers, down_edges, down_senders, down_receivers,
    edge_in_weight, edge_in_bias, edge_out_weight, edge_out_bias, edge_gain, edge_shift,
    node_in_weight, node_in_bias, node_out_weight, node_out_bias, node_gain, node_shift,
):
    groups, patches = lax.axis_size("group"), lax.axis_size("patch")
    count, width = fine_nodes.shape
    owned = coarse_nodes.shape[0]
    slots = fine_edges.shape[0]
    crossing = up_edges.shape[0]
    everywhere = groups * patches * owned
    side = everywhere // 2
    steps = slots // TILE
    lanes = lambda index: index.reshape(-1, 128)
    row = lambda vector: vector.reshape(1, -1)
    vm = pl.BlockSpec(memory_space=pltpu.VMEM)
    anywhere = pl.BlockSpec(memory_space=pl.ANY)
    outs = (fine_nodes, coarse_nodes, fine_edges, up_edges, down_edges)
    rows = lambda n, dtype=BF: pltpu.VMEM((n, width), dtype)
    dma = pltpu.SemaphoreType.DMA
    indices = tuple(
        lanes(a)
        for a in (fine_senders, fine_receivers, up_senders, up_receivers, down_senders, down_receivers)
    )
    vectors = tuple(
        row(a)
        for a in (
            edge_in_bias, edge_out_bias, edge_gain, edge_shift,
            node_in_bias, node_out_bias, node_gain, node_shift,
        )
    )
    results = pl.pallas_call(
        functools.partial(kernel, groups, patches),
        out_shape=tuple(pltpu.VMEM(a.shape, a.dtype) for a in outs),
        in_specs=[pl.BlockSpec(memory_space=pltpu.SMEM)] + [anywhere] * 23,
        out_specs=(vm,) * 5,
        scratch_shapes=[
            rows(count + 2 * RIM),
            rows(3 * width), rows(width), rows(2 * width), rows(width),
            rows(count + 2 * RIM), rows(count), rows(slots, F32), rows(count, F32),
            rows(everywhere), rows(everywhere), rows(side), rows(side), rows(side),
            rows(crossing, F32), rows(crossing, F32),
            *(pltpu.VMEM(a.shape, a.dtype) for a in indices + vectors),
            dma((8 + steps,)), dma((len(indices + vectors),)), dma((2,)), dma((2,)),
            dma(()), dma((4,)), dma((8,)), dma((8,)), dma(()), dma(()),
        ],
        compiler_params=pltpu.CompilerParams(
            vmem_limit_bytes=50 * 1024 * 1024, collective_id=0, has_side_effects=True
        ),
    )(
        fine_live, *indices, *vectors,
        fine_nodes, coarse_nodes, fine_edges, up_edges, down_edges,
        edge_in_weight, edge_out_weight, node_in_weight, node_out_weight,
    )
    return pl.pallas_call(
        writer,
        out_shape=tuple(jax.ShapeDtypeStruct(a.shape, a.dtype) for a in outs),
        in_specs=[vm] * 5,
        out_specs=(anywhere,) * 5,
        scratch_shapes=[dma((slots // 512 + count // 512 + 3,))],
        compiler_params=pltpu.CompilerParams(vmem_limit_bytes=2**20),
    )(*results)


def solution(mesh):
    rows, vector = P(BOTH, None), P(BOTH)
    return jax.shard_map(
        body,
        mesh=mesh,
        in_specs=(rows,) * 3 + (vector,) * 3 + (rows, vector, vector) * 2 + (P(),) * 12,
        out_specs=(rows,) * 5,
        check_vma=False,
    )
```

```python
import functools

import jax
import jax.numpy as jnp
from jax import lax
from jax.experimental import pallas as pl
from jax.experimental.pallas import tpu as pltpu
from jax.sharding import PartitionSpec as P

RIM = 128
BF = jnp.bfloat16
F32 = jnp.float32
TILE = 1024
BOTH = ("group", "patch")
MESH = pl.DeviceIdType.MESH


def dot(a, b):
    return jnp.dot(a, b, preferred_element_type=F32)


def dot_t(a, b):
    return lax.dot_general(a, b, (((0,), (0,)), ((), ())), preferred_element_type=F32)


def one_hot_t(rows, index):
    iota = lax.broadcasted_iota(jnp.int32, (rows, 128), 0)
    blocks = [
        jnp.where(iota == index[j : j + 1, :], 1.0, 0.0).astype(BF) for j in range(index.shape[0])
    ]
    return jnp.concatenate(blocks, axis=1)


def silu(u):
    half = 0.5 * u
    return half + half * jnp.tanh(half)


def centred(matrix):
    wide = matrix.astype(F32)
    return (wide - jnp.mean(wide, axis=-1, keepdims=True)).astype(matrix.dtype)


def tail(pre, out_weight, out_bias, gain, shift):
    r = dot(silu(pre).astype(BF), out_weight[...]) + out_bias[...]
    spread = jnp.mean(r * r, axis=-1, keepdims=True)
    return r * lax.rsqrt(spread + 1e-05) * gain[...] + shift[...]


def kernel(
    groups, patches,
    live_in, senders_in, receivers_in, up_send_in, up_recv_in, down_send_in, down_recv_in,
    b1_in, b2_in, gain_in, shift_in, c1_in, c2_in, node_gain_in, node_shift_in,
    nodes, coarse, edges, up, down, w1_in, w2_in, v1_in, v2_in,
    fine_new, coarse_new, eb, ub, db,
    win, w1, w2, v1, v2, by_sender, by_receiver, pre, sums, table, part, beside, half,
    landed, up_pre,
    senders, receivers, up_send, up_recv, down_send, down_recv,
    b1, b2, gain, shift, c1, c2, node_gain, node_shift,
    by_rim, live,
    load, few, rim_sent, rim_got, spread_sent, spread_got, twin_sent, twin_got, home_sent, home_got,
):
    count, width = nodes.shape
    slots = edges.shape[0]
    owned = coarse.shape[0]
    g, p = lax.axis_index("group"), lax.axis_index("patch")
    core, high = lax.rem(g, 2), g // 2
    chips = groups // 2 * patches
    side = chips * owned
    me = high * patches + p
    planes = 4
    plane = chips // planes
    mine_y, mine_xz = me // plane, lax.rem(me, plane)
    band = plane * owned
    twin = (high * 2 + 1 - core, p)
    mine = pl.ds(pl.multiple_of(me * owned, owned), owned)

    def in_plane(ahead, action):
        y = lax.rem(mine_y + ahead, planes)
        group = y * plane // patches * 2 + core
        first = lax.rem(y * plane, patches)

        def one(k, carry):
            action(y * plane + k, (group, first + k))
            return carry

        lax.fori_loop(mine_xz if ahead else mine_xz + 1, plane, one, 0)
        lax.fori_loop(0, mine_xz, one, 0)

    def ahead_rows(ahead, start=0):
        y = lax.rem(mine_y + ahead + planes, planes)
        return pl.ds(pl.multiple_of(y * band + start, band), band)

    def remote(source, target, sent, got, device):
        return pltpu.make_async_remote_copy(
            source, target, sent, got, device_id=device, device_id_type=MESH
        )

    def settle(ref, sem):
        pltpu.make_async_copy(ref, ref, sem).wait()

    barrier = pltpu.get_barrier_semaphore()

    def greet(other, device):
        pl.semaphore_signal(barrier, inc=1, device_id=device, device_id_type=MESH)

    greet(0, twin)
    for ahead in range(planes):
        in_plane(ahead, greet)

    steps = slots // TILE
    early = steps - 1
    tile = lambda t: pl.ds(pl.multiple_of(t * TILE, TILE), TILE)
    own_rows = slice(RIM, RIM + count)
    get_nodes = pltpu.make_async_copy(nodes, win.at[pl.ds(RIM, count)], load.at[0])
    get_w1 = pltpu.make_async_copy(w1_in, w1, load.at[1])
    get_own = pltpu.make_async_copy(coarse, table.at[mine], load.at[2])
    get_w2 = pltpu.make_async_copy(w2_in, w2, load.at[3])
    get_up = pltpu.make_async_copy(up, ub, load.at[4])
    get_down = pltpu.make_async_copy(down, db, load.at[5])
    get_v1 = pltpu.make_async_copy(v1_in, v1, load.at[6])
    get_v2 = pltpu.make_async_copy(v2_in, v2, load.at[7])
    get_edges = lambda t: pltpu.make_async_copy(edges.at[tile(t)], eb.at[tile(t)], load.at[8 + t])
    small = (
        (live_in, live), (senders_in, senders), (receivers_in, receivers), (up_send_in, up_send),
        (up_recv_in, up_recv), (down_send_in, down_send), (down_recv_in, down_recv),
        (b1_in, b1), (b2_in, b2), (gain_in, gain), (shift_in, shift), (c1_in, c1), (c2_in, c2),
        (node_gain_in, node_gain), (node_shift_in, node_shift),
    )
    small = [pltpu.make_async_copy(a, b, few.at[i]) for i, (a, b) in enumerate(small)]
    get_nodes.start()
    get_w1.start()
    get_own.start()

    before = (g, lax.rem(p + patches - 1, patches))
    after = (g, lax.rem(p + 1, patches))
    to_after = remote(
        nodes.at[pl.ds(count - RIM, RIM)], win.at[pl.ds(0, RIM)], rim_sent.at[0], rim_got.at[0], after
    )
    to_before = remote(
        nodes.at[pl.ds(0, RIM)], win.at[pl.ds(RIM + count, RIM)], rim_sent.at[1], rim_got.at[1], before
    )
    same = pl.ds(0, side)
    other_side = pl.ds(side, side)
    table_over = lambda ahead: remote(
        table.at[ahead_rows(-ahead)],
        table.at[ahead_rows(-ahead, side)],
        twin_sent.at[ahead],
        twin_got.at[ahead],
        twin,
    )
    part_over = lambda ahead: remote(
        part.at[ahead_rows(ahead, side)],
        beside.at[ahead_rows(ahead)],
        twin_sent.at[planes + ahead],
        twin_got.at[planes + ahead],
        twin,
    )
    all_but_one = pl.ds(0, side - owned)
    arriving = lambda ahead: pl.ds(0, band if ahead else band - owned)

    def spread(ahead):
        def send(other, device):
            remote(coarse, table.at[mine], spread_sent, spread_got.at[ahead], device).start()

        in_plane(ahead, send)

    with jax.named_scope("wait_bar"):
        pl.semaphore_wait(barrier, chips)
    for ahead in range(planes):
        spread(ahead)
    get_up.start()
    for copy in small:
        copy.start()
    get_down.start()
    for t in range(early):
        get_edges(t).start()
    get_w2.start()
    get_edges(early).start()
    get_v1.start()
    get_v2.start()

    def local_row(index):
        owner, inner = index // (patches * owned), lax.rem(index, patches * owned)
        away = jnp.where(lax.rem(owner, 2) == core, 0, side)
        return owner // 2 * (patches * owned) + inner + away

    with jax.named_scope("wait_load"):
        get_nodes.wait()
        get_w1.wait()
    w_edge, w_send, w_recv = (w1.at[pl.ds(i * width, width)] for i in range(3))
    by_sender[...] = dot(win[own_rows, :], w_send[...]).astype(BF)
    by_receiver[...] = dot(win[own_rows, :], w_recv[...]).astype(BF)
    for copy in small:
        copy.wait()
    get_up.wait()
    up_pre[...] = (
        dot(ub[...], w_edge[...])
        + b1[...]
        + dot_t(one_hot_t(count, up_send[...]), by_sender[...])
    )
    blocks = TILE // 128
    index_rows = lambda t: pl.ds(pl.multiple_of(t * blocks, blocks), blocks)

    def main(t):
        get_edges(t).wait()
        pre[tile(t), :] = (
            dot(eb[tile(t), :], w_edge[...])
            + b1[...]
            + dot_t(one_hot_t(count, senders[index_rows(t), :] - RIM), by_sender[...])
            + dot_t(one_hot_t(count, receivers[index_rows(t), :]), by_receiver[...])
        )

    def early_step(t, carry):
        main(t)
        return carry

    def pass_on(ahead):
        with jax.named_scope("wait_spread"):
            settle(table.at[arriving(ahead)], spread_got.at[ahead])
        table_over(ahead).start()

    lax.fori_loop(0, early, early_step, 0)
    get_own.wait()
    get_w2.wait()
    pass_on(0)
    pass_on(1)
    main(early)
    w2[...] = centred(w2[...])
    b2[...] = centred(b2[...])
    pass_on(2)
    pass_on(3)
    to_after.start()
    to_before.start()
    near, far = slice(0, side), slice(side, 2 * side)
    with jax.named_scope("up"):
        to_coarse = one_hot_t(2 * side, local_row(up_recv[...]))
        picked = dot_t(to_coarse[near], table[near, :])
        with jax.named_scope("wait_twin"):
            for ahead in range(planes):
                table_over(ahead).wait_recv()
        picked = (picked + dot_t(to_coarse[far], table[far, :])).astype(BF)
        new = tail(up_pre[...] + dot(picked, w_recv[...]), w2, b2, gain, shift)
        new = (ub[...].astype(F32) + new).astype(BF)
        ub[...] = new
        part[far, :] = dot(to_coarse[far], new).astype(BF)
        for ahead in range(planes):
            part_over(ahead).start()
        part[near, :] = dot(to_coarse[near], new).astype(BF)

    with jax.named_scope("home"):
        for ahead in range(planes):
            part_over(ahead).wait_recv()
            rows = ahead_rows(ahead)
            half[rows, :] = (part[rows, :].astype(F32) + beside[rows, :].astype(F32)).astype(BF)

            def home(other, device):
                block = pl.ds(pl.multiple_of(other * owned, owned), owned)
                remote(half.at[block], landed.at[mine], home_sent, home_got, device).start()

            in_plane(ahead, home)
        landed[mine, :] = half[mine, :]

    with jax.named_scope("down"):
        get_down.wait()
        picked = dot_t(one_hot_t(2 * side, local_row(down_send[...])), table[...]).astype(BF)
        to_fine = one_hot_t(count, down_recv[...])
        full = (
            dot(db[...], w_edge[...])
            + b1[...]
            + dot_t(to_fine, by_receiver[...])
            + dot(picked, w_send[...])
        )
        new = tail(full, w2, b2, gain, shift)
        new = (db[...].astype(F32) + new).astype(BF)
        db[...] = new
        sums[...] = dot(to_fine, new)

    with jax.named_scope("wait_rim"):
        to_after.wait_recv()
        to_before.wait_recv()
    by_rim[0:RIM, :] = dot(win[0:RIM, :], w_send[...]).astype(BF)
    by_rim[RIM:, :] = dot(win[RIM + count :, :], w_send[...]).astype(BF)

    def finished(t):
        send_row = senders[index_rows(t), :]
        rim_row = jnp.where(
            send_row < RIM, send_row, jnp.where(send_row < RIM + count, -1, send_row - count)
        )
        new = tail(
            pre[tile(t), :] + dot_t(one_hot_t(2 * RIM, rim_row), by_rim[...]), w2, b2, gain, shift
        )
        slot = lax.broadcasted_iota(jnp.int32, (TILE, 1), 0) + t * TILE
        return (eb[tile(t), :].astype(F32) + jnp.where(slot < live[0], new, 0.0)).astype(BF)

    def step(i, carry):
        first, second = finished(2 * i), finished(2 * i + 1)
        eb[tile(2 * i), :] = first
        eb[tile(2 * i + 1), :] = second
        rows = pl.ds(pl.multiple_of(2 * i * blocks, 2 * blocks), 2 * blocks)
        index = receivers[rows, :]
        slot = (
            lax.broadcasted_iota(jnp.int32, index.shape, 0) * 128
            + lax.broadcasted_iota(jnp.int32, index.shape, 1)
            + 2 * i * TILE
        )
        sums[...] += dot(
            one_hot_t(count, jnp.where(slot < live[0], index, -1)),
            jnp.concatenate([first, second], axis=0),
        )
        return carry

    with jax.named_scope("tails"):
        lax.fori_loop(0, steps // 2, step, 0)
    get_v1.wait()
    get_v2.wait()
    v2[...] = centred(v2[...])
    c2[...] = centred(c2[...])

    def node_net(old, summed):
        inner = dot(old, v1[0:width, :]) + c1[...] + dot(summed, v1[width : 2 * width, :])
        return (old.astype(F32) + tail(inner, v2, c2, node_gain, node_shift)).astype(BF)

    with jax.named_scope("node"):
        fine_new[...] = node_net(win[own_rows, :], sums[...].astype(BF))

    with jax.named_scope("wait_home"):
        settle(landed.at[all_but_one], home_got)
    with jax.named_scope("ends"):
        arrived = jnp.sum(landed[...].astype(F32).reshape(chips, owned, width), axis=0).astype(BF)
        coarse_new[...] = node_net(table[mine, :], arrived)
        to_after.wait_send()
        to_before.wait_send()
        settle(table.at[all_but_one], spread_sent)
        settle(half.at[all_but_one], home_sent)
        for ahead in range(planes):
            table_over(ahead).wait_send()
            part_over(ahead).wait_send()


def writer(fine, coarse, edges, up, down, *outs_and_sem):
    *outs, sem = outs_and_sem
    copies = []
    for source, target in zip((edges, fine, up, down, coarse), (outs[2], outs[0], *outs[3:], outs[1])):
        size = min(source.shape[0], 512)
        for at in range(0, source.shape[0], size):
            rows = pl.ds(at, size)
            copies.append(pltpu.make_async_copy(source.at[rows], target.at[rows], sem.at[len(copies)]))
    for copy in copies:
        copy.start()
    for copy in copies:
        copy.wait()


def body(
    fine_nodes, coarse_nodes, fine_edges, fine_senders, fine_receivers, fine_live,
    up_edges, up_senders, up_receivers, down_edges, down_senders, down_receivers,
    edge_in_weight, edge_in_bias, edge_out_weight, edge_out_bias, edge_gain, edge_shift,
    node_in_weight, node_in_bias, node_out_weight, node_out_bias, node_gain, node_shift,
):
    groups, patches = lax.axis_size("group"), lax.axis_size("patch")
    count, width = fine_nodes.shape
    owned = coarse_nodes.shape[0]
    slots = fine_edges.shape[0]
    crossing = up_edges.shape[0]
    everywhere = groups * patches * owned
    side = everywhere // 2
    steps = slots // TILE
    lanes = lambda index: index.reshape(-1, 128)
    row = lambda vector: vector.reshape(1, -1)
    vm = pl.BlockSpec(memory_space=pltpu.VMEM)
    anywhere = pl.BlockSpec(memory_space=pl.ANY)
    outs = (fine_nodes, coarse_nodes, fine_edges, up_edges, down_edges)
    rows = lambda n, dtype=BF: pltpu.VMEM((n, width), dtype)
    dma = pltpu.SemaphoreType.DMA
    indices = tuple(
        lanes(a)
        for a in (fine_senders, fine_receivers, up_senders, up_receivers, down_senders, down_receivers)
    )
    vectors = tuple(
        row(a)
        for a in (
            edge_in_bias, edge_out_bias, edge_gain, edge_shift,
            node_in_bias, node_out_bias, node_gain, node_shift,
        )
    )
    results = pl.pallas_call(
        functools.partial(kernel, groups, patches),
        out_shape=tuple(pltpu.VMEM(a.shape, a.dtype) for a in outs),
        in_specs=[anywhere] * 24,
        out_specs=(vm,) * 5,
        scratch_shapes=[
            rows(count + 2 * RIM),
            rows(3 * width), rows(width), rows(2 * width), rows(width),
            rows(count), rows(count), rows(slots, F32), rows(count, F32),
            rows(everywhere), rows(everywhere), rows(side), rows(side), rows(side),
            rows(crossing, F32),
            *(pltpu.VMEM(a.shape, a.dtype) for a in indices + vectors),
            rows(2 * RIM), pltpu.SMEM((1,), jnp.int32),
            dma((8 + steps,)), dma((len(indices + vectors) + 1,)), dma((2,)), dma((2,)),
            dma(()), dma((4,)), dma((8,)), dma((8,)), dma(()), dma(()),
        ],
        compiler_params=pltpu.CompilerParams(
            vmem_limit_bytes=50 * 1024 * 1024, collective_id=0, has_side_effects=True
        ),
    )(
        fine_live, *indices, *vectors,
        fine_nodes, coarse_nodes, fine_edges, up_edges, down_edges,
        edge_in_weight, edge_out_weight, node_in_weight, node_out_weight,
    )
    return pl.pallas_call(
        writer,
        out_shape=tuple(jax.ShapeDtypeStruct(a.shape, a.dtype) for a in outs),
        in_specs=[vm] * 5,
        out_specs=(anywhere,) * 5,
        scratch_shapes=[dma((slots // 512 + count // 512 + 3,))],
        compiler_params=pltpu.CompilerParams(vmem_limit_bytes=2**20),
    )(*results)


def solution(mesh):
    rows, vector = P(BOTH, None), P(BOTH)
    return jax.shard_map(
        body,
        mesh=mesh,
        in_specs=(rows,) * 3 + (vector,) * 3 + (rows, vector, vector) * 2 + (P(),) * 12,
        out_specs=(rows,) * 5,
        check_vma=False,
    )
```

```python
import functools

import jax
import jax.numpy as jnp
from jax import lax
from jax.experimental import pallas as pl
from jax.experimental.pallas import tpu as pltpu
from jax.sharding import PartitionSpec as P

RIM = 128
BF = jnp.bfloat16
F32 = jnp.float32
TILE = 1024
BOTH = ("group", "patch")
MESH = pl.DeviceIdType.MESH


def dot(a, b):
    return jnp.dot(a, b, preferred_element_type=F32)


def dot_t(a, b):
    return lax.dot_general(a, b, (((0,), (0,)), ((), ())), preferred_element_type=F32)


def one_hot_t(rows, index):
    iota = lax.broadcasted_iota(jnp.int32, (rows, 128), 0)
    blocks = [
        jnp.where(iota == index[j : j + 1, :], 1.0, 0.0).astype(BF) for j in range(index.shape[0])
    ]
    return jnp.concatenate(blocks, axis=1)


def silu(u):
    half = 0.5 * u
    return half + half * jnp.tanh(half)


def centred(matrix):
    wide = matrix.astype(F32)
    return (wide - jnp.mean(wide, axis=-1, keepdims=True)).astype(matrix.dtype)


def tail(pre, out_weight, out_bias, gain, shift):
    r = dot(silu(pre).astype(BF), out_weight[...]) + out_bias[...]
    spread = jnp.mean(r * r, axis=-1, keepdims=True)
    return r * lax.rsqrt(spread + 1e-05) * gain[...] + shift[...]


def kernel(
    groups, patches,
    live_in, senders_in, receivers_in, up_send_in, up_recv_in, down_send_in, down_recv_in,
    b1_in, b2_in, gain_in, shift_in, c1_in, c2_in, node_gain_in, node_shift_in,
    nodes, coarse, edges, up, down, w1_in, w2_in, v1_in, v2_in,
    fine_new, coarse_new, eb, ub, db,
    win, w1, w2, v1, v2, by_sender, by_receiver, pre, sums, table, part, beside, half,
    landed, up_pre, down_pre,
    senders, receivers, up_send, up_recv, down_send, down_recv,
    b1, b2, gain, shift, c1, c2, node_gain, node_shift,
    by_rim, live,
    load, few, rim_sent, rim_got, spread_sent, spread_got, twin_sent, twin_got, home_sent, home_got,
):
    count, width = nodes.shape
    slots = edges.shape[0]
    owned = coarse.shape[0]
    g, p = lax.axis_index("group"), lax.axis_index("patch")
    core, high = lax.rem(g, 2), g // 2
    chips = groups // 2 * patches
    side = chips * owned
    me = high * patches + p
    planes = 4
    plane = chips // planes
    mine_y, mine_xz = me // plane, lax.rem(me, plane)
    band = plane * owned
    twin = (high * 2 + 1 - core, p)
    mine = pl.ds(pl.multiple_of(me * owned, owned), owned)

    def in_plane(ahead, action):
        y = lax.rem(mine_y + ahead, planes)
        group = y * plane // patches * 2 + core
        first = lax.rem(y * plane, patches)

        def one(k, carry):
            action(y * plane + k, (group, first + k))
            return carry

        lax.fori_loop(mine_xz if ahead else mine_xz + 1, plane, one, 0)
        lax.fori_loop(0, mine_xz, one, 0)

    def ahead_rows(ahead, start=0):
        y = lax.rem(mine_y + ahead + planes, planes)
        return pl.ds(pl.multiple_of(y * band + start, band), band)

    def remote(source, target, sent, got, device):
        return pltpu.make_async_remote_copy(
            source, target, sent, got, device_id=device, device_id_type=MESH
        )

    def settle(ref, sem):
        pltpu.make_async_copy(ref, ref, sem).wait()

    barrier = pltpu.get_barrier_semaphore()

    def greet(other, device):
        pl.semaphore_signal(barrier, inc=1, device_id=device, device_id_type=MESH)

    greet(0, twin)
    for ahead in range(planes):
        in_plane(ahead, greet)

    steps = slots // TILE
    early = steps - 1
    tile = lambda t: pl.ds(pl.multiple_of(t * TILE, TILE), TILE)
    own_rows = slice(RIM, RIM + count)
    get_nodes = pltpu.make_async_copy(nodes, win.at[pl.ds(RIM, count)], load.at[0])
    get_w1 = pltpu.make_async_copy(w1_in, w1, load.at[1])
    get_own = pltpu.make_async_copy(coarse, table.at[mine], load.at[2])
    get_w2 = pltpu.make_async_copy(w2_in, w2, load.at[3])
    get_up = pltpu.make_async_copy(up, ub, load.at[4])
    get_down = pltpu.make_async_copy(down, db, load.at[5])
    get_v1 = pltpu.make_async_copy(v1_in, v1, load.at[6])
    get_v2 = pltpu.make_async_copy(v2_in, v2, load.at[7])
    get_edges = lambda t: pltpu.make_async_copy(edges.at[tile(t)], eb.at[tile(t)], load.at[8 + t])
    small = (
        (live_in, live), (senders_in, senders), (receivers_in, receivers), (up_send_in, up_send),
        (up_recv_in, up_recv), (down_send_in, down_send), (down_recv_in, down_recv),
        (b1_in, b1), (b2_in, b2), (gain_in, gain), (shift_in, shift), (c1_in, c1), (c2_in, c2),
        (node_gain_in, node_gain), (node_shift_in, node_shift),
    )
    small = [pltpu.make_async_copy(a, b, few.at[i]) for i, (a, b) in enumerate(small)]
    get_nodes.start()
    get_w1.start()
    get_own.start()

    before = (g, lax.rem(p + patches - 1, patches))
    after = (g, lax.rem(p + 1, patches))
    to_after = remote(
        nodes.at[pl.ds(count - RIM, RIM)], win.at[pl.ds(0, RIM)], rim_sent.at[0], rim_got.at[0], after
    )
    to_before = remote(
        nodes.at[pl.ds(0, RIM)], win.at[pl.ds(RIM + count, RIM)], rim_sent.at[1], rim_got.at[1], before
    )
    same = pl.ds(0, side)
    other_side = pl.ds(side, side)
    table_over = lambda ahead: remote(
        table.at[ahead_rows(-ahead)],
        table.at[ahead_rows(-ahead, side)],
        twin_sent.at[ahead],
        twin_got.at[ahead],
        twin,
    )
    part_over = lambda ahead: remote(
        part.at[ahead_rows(ahead, side)],
        beside.at[ahead_rows(ahead)],
        twin_sent.at[planes + ahead],
        twin_got.at[planes + ahead],
        twin,
    )
    all_but_one = pl.ds(0, side - owned)
    arriving = lambda ahead: pl.ds(0, band if ahead else band - owned)

    def spread(ahead):
        def send(other, device):
            remote(table.at[mine], table.at[mine], spread_sent, spread_got.at[ahead], device).start()

        in_plane(ahead, send)

    with jax.named_scope("wait_load"):
        get_nodes.wait()
        get_w1.wait()
    get_up.start()
    for copy in small:
        copy.start()
    get_down.start()
    for t in range(early):
        get_edges(t).start()
    get_w2.start()
    get_edges(early).start()
    get_v1.start()
    get_v2.start()
    w_edge, w_send, w_recv = (w1.at[pl.ds(i * width, width)] for i in range(3))
    by_sender[...] = dot(win[own_rows, :], w_send[...]).astype(BF)
    by_receiver[...] = dot(win[own_rows, :], w_recv[...]).astype(BF)
    get_own.wait()
    with jax.named_scope("wait_bar"):
        pl.semaphore_wait(barrier, chips)
    for ahead in range(planes):
        spread(ahead)

    def local_row(index):
        owner, inner = index // (patches * owned), lax.rem(index, patches * owned)
        away = jnp.where(lax.rem(owner, 2) == core, 0, side)
        return owner // 2 * (patches * owned) + inner + away

    for copy in small:
        copy.wait()
    get_up.wait()
    up_pre[...] = (
        dot(ub[...], w_edge[...])
        + b1[...]
        + dot_t(one_hot_t(count, up_send[...]), by_sender[...])
    )
    blocks = TILE // 128
    index_rows = lambda t: pl.ds(pl.multiple_of(t * blocks, blocks), blocks)

    def main(t):
        get_edges(t).wait()
        pre[tile(t), :] = (
            dot(eb[tile(t), :], w_edge[...])
            + b1[...]
            + dot_t(one_hot_t(count, senders[index_rows(t), :] - RIM), by_sender[...])
            + dot_t(one_hot_t(count, receivers[index_rows(t), :]), by_receiver[...])
        )

    def early_step(t, carry):
        main(t)
        return carry

    def pass_on(ahead):
        with jax.named_scope("wait_spread"):
            settle(table.at[arriving(ahead)], spread_got.at[ahead])
        table_over(ahead).start()

    lax.fori_loop(0, early, early_step, 0)
    get_w2.wait()
    pass_on(0)
    pass_on(1)
    main(early)
    w2[...] = centred(w2[...])
    b2[...] = centred(b2[...])
    pass_on(2)
    pass_on(3)
    to_after.start()
    to_before.start()
    get_down.wait()
    down_pre[...] = (
        dot(db[...], w_edge[...])
        + b1[...]
        + dot_t(one_hot_t(count, down_recv[...]), by_receiver[...])
    )
    near, far = slice(0, side), slice(side, 2 * side)
    with jax.named_scope("up"):
        to_coarse = one_hot_t(2 * side, local_row(up_recv[...]))
        picked = dot_t(to_coarse[near], table[near, :])
        with jax.named_scope("wait_twin"):
            for ahead in range(planes):
                table_over(ahead).wait_recv()
        picked = (picked + dot_t(to_coarse[far], table[far, :])).astype(BF)
        new = tail(up_pre[...] + dot(picked, w_recv[...]), w2, b2, gain, shift)
        new = (ub[...].astype(F32) + new).astype(BF)
        ub[...] = new
        part[far, :] = dot(to_coarse[far], new).astype(BF)
        for ahead in range(planes):
            part_over(ahead).start()
        part[near, :] = dot(to_coarse[near], new).astype(BF)

    with jax.named_scope("home"):
        for ahead in range(planes):
            part_over(ahead).wait_recv()
            rows = ahead_rows(ahead)
            half[rows, :] = (part[rows, :].astype(F32) + beside[rows, :].astype(F32)).astype(BF)

            def home(other, device):
                block = pl.ds(pl.multiple_of(other * owned, owned), owned)
                remote(half.at[block], landed.at[mine], home_sent, home_got, device).start()

            in_plane(ahead, home)
        landed[mine, :] = half[mine, :]

    with jax.named_scope("down"):
        picked = dot_t(one_hot_t(2 * side, local_row(down_send[...])), table[...]).astype(BF)
        to_fine = one_hot_t(count, down_recv[...])
        new = tail(down_pre[...] + dot(picked, w_send[...]), w2, b2, gain, shift)
        new = (db[...].astype(F32) + new).astype(BF)
        db[...] = new
        sums[...] = dot(to_fine, new)

    with jax.named_scope("wait_rim"):
        to_after.wait_recv()
        to_before.wait_recv()
    by_rim[0:RIM, :] = dot(win[0:RIM, :], w_send[...]).astype(BF)
    by_rim[RIM:, :] = dot(win[RIM + count :, :], w_send[...]).astype(BF)

    def finished(t):
        send_row = senders[index_rows(t), :]
        rim_row = jnp.where(
            send_row < RIM, send_row, jnp.where(send_row < RIM + count, -1, send_row - count)
        )
        new = tail(
            pre[tile(t), :] + dot_t(one_hot_t(2 * RIM, rim_row), by_rim[...]), w2, b2, gain, shift
        )
        slot = lax.broadcasted_iota(jnp.int32, (TILE, 1), 0) + t * TILE
        return (eb[tile(t), :].astype(F32) + jnp.where(slot < live[0], new, 0.0)).astype(BF)

    def step(i, carry):
        first, second = finished(2 * i), finished(2 * i + 1)
        eb[tile(2 * i), :] = first
        eb[tile(2 * i + 1), :] = second
        rows = pl.ds(pl.multiple_of(2 * i * blocks, 2 * blocks), 2 * blocks)
        index = receivers[rows, :]
        slot = (
            lax.broadcasted_iota(jnp.int32, index.shape, 0) * 128
            + lax.broadcasted_iota(jnp.int32, index.shape, 1)
            + 2 * i * TILE
        )
        sums[...] += dot(
            one_hot_t(count, jnp.where(slot < live[0], index, -1)),
            jnp.concatenate([first, second], axis=0),
        )
        return carry

    with jax.named_scope("tails"):
        lax.fori_loop(0, steps // 2, step, 0)
    get_v1.wait()
    get_v2.wait()
    v2[...] = centred(v2[...])
    c2[...] = centred(c2[...])

    def node_net(old, summed):
        inner = dot(old, v1[0:width, :]) + c1[...] + dot(summed, v1[width : 2 * width, :])
        return (old.astype(F32) + tail(inner, v2, c2, node_gain, node_shift)).astype(BF)

    with jax.named_scope("node"):
        fine_new[...] = node_net(win[own_rows, :], sums[...].astype(BF))

    with jax.named_scope("wait_home"):
        settle(landed.at[all_but_one], home_got)
    with jax.named_scope("ends"):
        arrived = jnp.sum(landed[...].astype(F32).reshape(chips, owned, width), axis=0).astype(BF)
        coarse_new[...] = node_net(table[mine, :], arrived)
        to_after.wait_send()
        to_before.wait_send()
        settle(table.at[all_but_one], spread_sent)
        settle(half.at[all_but_one], home_sent)
        for ahead in range(planes):
            table_over(ahead).wait_send()
            part_over(ahead).wait_send()


def writer(fine, coarse, edges, up, down, *outs_and_sem):
    *outs, sem = outs_and_sem
    copies = []
    for source, target in zip((edges, fine, up, down, coarse), (outs[2], outs[0], *outs[3:], outs[1])):
        size = min(source.shape[0], 512)
        for at in range(0, source.shape[0], size):
            rows = pl.ds(at, size)
            copies.append(pltpu.make_async_copy(source.at[rows], target.at[rows], sem.at[len(copies)]))
    for copy in copies:
        copy.start()
    for copy in copies:
        copy.wait()


def body(
    fine_nodes, coarse_nodes, fine_edges, fine_senders, fine_receivers, fine_live,
    up_edges, up_senders, up_receivers, down_edges, down_senders, down_receivers,
    edge_in_weight, edge_in_bias, edge_out_weight, edge_out_bias, edge_gain, edge_shift,
    node_in_weight, node_in_bias, node_out_weight, node_out_bias, node_gain, node_shift,
):
    groups, patches = lax.axis_size("group"), lax.axis_size("patch")
    count, width = fine_nodes.shape
    owned = coarse_nodes.shape[0]
    slots = fine_edges.shape[0]
    crossing = up_edges.shape[0]
    everywhere = groups * patches * owned
    side = everywhere // 2
    steps = slots // TILE
    lanes = lambda index: index.reshape(-1, 128)
    row = lambda vector: vector.reshape(1, -1)
    vm = pl.BlockSpec(memory_space=pltpu.VMEM)
    anywhere = pl.BlockSpec(memory_space=pl.ANY)
    outs = (fine_nodes, coarse_nodes, fine_edges, up_edges, down_edges)
    rows = lambda n, dtype=BF: pltpu.VMEM((n, width), dtype)
    dma = pltpu.SemaphoreType.DMA
    indices = tuple(
        lanes(a)
        for a in (fine_senders, fine_receivers, up_senders, up_receivers, down_senders, down_receivers)
    )
    vectors = tuple(
        row(a)
        for a in (
            edge_in_bias, edge_out_bias, edge_gain, edge_shift,
            node_in_bias, node_out_bias, node_gain, node_shift,
        )
    )
    results = pl.pallas_call(
        functools.partial(kernel, groups, patches),
        out_shape=tuple(pltpu.VMEM(a.shape, a.dtype) for a in outs),
        in_specs=[anywhere] * 24,
        out_specs=(vm,) * 5,
        scratch_shapes=[
            rows(count + 2 * RIM),
            rows(3 * width), rows(width), rows(2 * width), rows(width),
            rows(count), rows(count), rows(slots, F32), rows(count, F32),
            rows(everywhere), rows(everywhere), rows(side), rows(side), rows(side),
            rows(crossing, F32), rows(crossing, F32),
            *(pltpu.VMEM(a.shape, a.dtype) for a in indices + vectors),
            rows(2 * RIM), pltpu.SMEM((1,), jnp.int32),
            dma((8 + steps,)), dma((len(indices + vectors) + 1,)), dma((2,)), dma((2,)),
            dma(()), dma((4,)), dma((8,)), dma((8,)), dma(()), dma(()),
        ],
        compiler_params=pltpu.CompilerParams(
            vmem_limit_bytes=50 * 1024 * 1024, collective_id=0, has_side_effects=True
        ),
    )(
        fine_live, *indices, *vectors,
        fine_nodes, coarse_nodes, fine_edges, up_edges, down_edges,
        edge_in_weight, edge_out_weight, node_in_weight, node_out_weight,
    )
    return pl.pallas_call(
        writer,
        out_shape=tuple(jax.ShapeDtypeStruct(a.shape, a.dtype) for a in outs),
        in_specs=[vm] * 5,
        out_specs=(anywhere,) * 5,
        scratch_shapes=[dma((slots // 512 + count // 512 + 3,))],
        compiler_params=pltpu.CompilerParams(vmem_limit_bytes=2**20),
    )(*results)


def solution(mesh):
    rows, vector = P(BOTH, None), P(BOTH)
    return jax.shard_map(
        body,
        mesh=mesh,
        in_specs=(rows,) * 3 + (vector,) * 3 + (rows, vector, vector) * 2 + (P(),) * 12,
        out_specs=(rows,) * 5,
        check_vma=False,
    )
```

```python
import functools

import jax
import jax.numpy as jnp
from jax import lax
from jax.experimental import pallas as pl
from jax.experimental.pallas import tpu as pltpu
from jax.sharding import PartitionSpec as P

RIM = 128
BF = jnp.bfloat16
F32 = jnp.float32
TILE = 1024
BOTH = ("group", "patch")
MESH = pl.DeviceIdType.MESH


def dot(a, b):
    return jnp.dot(a, b, preferred_element_type=F32)


def dot_t(a, b):
    return lax.dot_general(a, b, (((0,), (0,)), ((), ())), preferred_element_type=F32)


def one_hot_t(rows, index):
    iota = lax.broadcasted_iota(jnp.int32, (rows, 128), 0)
    blocks = [
        jnp.where(iota == index[j : j + 1, :], 1.0, 0.0).astype(BF) for j in range(index.shape[0])
    ]
    return jnp.concatenate(blocks, axis=1)


def silu(u):
    half = 0.5 * u
    return half + half * jnp.tanh(half)


def centred(matrix):
    wide = matrix.astype(F32)
    return (wide - jnp.mean(wide, axis=-1, keepdims=True)).astype(matrix.dtype)


def tail(pre, out_weight, out_bias, gain, shift):
    r = dot(silu(pre).astype(BF), out_weight[...]) + out_bias[...]
    spread = jnp.mean(r * r, axis=-1, keepdims=True)
    return r * lax.rsqrt(spread + 1e-05) * gain[...] + shift[...]


def kernel(
    groups, patches,
    live_in, senders_in, receivers_in, up_send_in, up_recv_in, down_send_in, down_recv_in,
    b1_in, b2_in, gain_in, shift_in, c1_in, c2_in, node_gain_in, node_shift_in,
    nodes, coarse, edges, up, down, w1_in, w2_in, v1_in, v2_in,
    fine_new, coarse_new, eb, ub, db,
    win, w1, w2, v1, v2, by_sender, by_receiver, pre, sums, table, part, beside, half,
    landed, up_pre,
    senders, receivers, up_send, up_recv, down_send, down_recv,
    b1, b2, gain, shift, c1, c2, node_gain, node_shift,
    by_rim, live,
    load, few, rim_sent, rim_got, spread_sent, spread_got, twin_sent, twin_got, home_sent, home_got,
):
    count, width = nodes.shape
    slots = edges.shape[0]
    owned = coarse.shape[0]
    g, p = lax.axis_index("group"), lax.axis_index("patch")
    core, high = lax.rem(g, 2), g // 2
    chips = groups // 2 * patches
    side = chips * owned
    me = high * patches + p
    planes = 4
    plane = chips // planes
    mine_y, mine_xz = me // plane, lax.rem(me, plane)
    band = plane * owned
    twin = (high * 2 + 1 - core, p)
    mine = pl.ds(pl.multiple_of(me * owned, owned), owned)

    def in_plane(ahead, action):
        y = lax.rem(mine_y + ahead, planes)
        group = y * plane // patches * 2 + core
        first = lax.rem(y * plane, patches)

        def one(k, carry):
            action(y * plane + k, (group, first + k))
            return carry

        lax.fori_loop(mine_xz if ahead else mine_xz + 1, plane, one, 0)
        lax.fori_loop(0, mine_xz, one, 0)

    def ahead_rows(ahead, start=0):
        y = lax.rem(mine_y + ahead + planes, planes)
        return pl.ds(pl.multiple_of(y * band + start, band), band)

    def remote(source, target, sent, got, device):
        return pltpu.make_async_remote_copy(
            source, target, sent, got, device_id=device, device_id_type=MESH
        )

    def settle(ref, sem):
        pltpu.make_async_copy(ref, ref, sem).wait()

    barrier = pltpu.get_barrier_semaphore()

    def greet(other, device):
        pl.semaphore_signal(barrier, inc=1, device_id=device, device_id_type=MESH)

    greet(0, twin)
    for ahead in range(planes):
        in_plane(ahead, greet)

    steps = slots // TILE
    early = steps - 1
    tile = lambda t: pl.ds(pl.multiple_of(t * TILE, TILE), TILE)
    own_rows = slice(RIM, RIM + count)
    get_nodes = pltpu.make_async_copy(nodes, win.at[pl.ds(RIM, count)], load.at[0])
    get_w1 = pltpu.make_async_copy(w1_in, w1, load.at[1])
    get_own = pltpu.make_async_copy(coarse, table.at[mine], load.at[2])
    get_w2 = pltpu.make_async_copy(w2_in, w2, load.at[3])
    get_up = pltpu.make_async_copy(up, ub, load.at[4])
    get_down = pltpu.make_async_copy(down, db, load.at[5])
    get_v1 = pltpu.make_async_copy(v1_in, v1, load.at[6])
    get_v2 = pltpu.make_async_copy(v2_in, v2, load.at[7])
    get_edges = lambda t: pltpu.make_async_copy(edges.at[tile(t)], eb.at[tile(t)], load.at[8 + t])
    small = (
        (live_in, live), (senders_in, senders), (receivers_in, receivers), (up_send_in, up_send),
        (up_recv_in, up_recv), (down_send_in, down_send), (down_recv_in, down_recv),
        (b1_in, b1), (b2_in, b2), (gain_in, gain), (shift_in, shift), (c1_in, c1), (c2_in, c2),
        (node_gain_in, node_gain), (node_shift_in, node_shift),
    )
    small = [pltpu.make_async_copy(a, b, few.at[i]) for i, (a, b) in enumerate(small)]
    get_nodes.start()
    get_w1.start()
    get_own.start()

    before = (g, lax.rem(p + patches - 1, patches))
    after = (g, lax.rem(p + 1, patches))
    to_after = remote(
        nodes.at[pl.ds(count - RIM, RIM)], win.at[pl.ds(0, RIM)], rim_sent.at[0], rim_got.at[0], after
    )
    to_before = remote(
        nodes.at[pl.ds(0, RIM)], win.at[pl.ds(RIM + count, RIM)], rim_sent.at[1], rim_got.at[1], before
    )
    same = pl.ds(0, side)
    other_side = pl.ds(side, side)
    table_over = lambda ahead: remote(
        table.at[ahead_rows(-ahead)],
        table.at[ahead_rows(-ahead, side)],
        twin_sent.at[ahead],
        twin_got.at[ahead],
        twin,
    )
    part_over = lambda ahead: remote(
        part.at[ahead_rows(ahead, side)],
        beside.at[ahead_rows(ahead)],
        twin_sent.at[planes + ahead],
        twin_got.at[planes + ahead],
        twin,
    )
    all_but_one = pl.ds(0, side - owned)
    arriving = lambda ahead: pl.ds(0, band if ahead else band - owned)

    def spread(ahead):
        def send(other, device):
            remote(table.at[mine], table.at[mine], spread_sent, spread_got.at[ahead], device).start()

        in_plane(ahead, send)

    get_own.wait()
    with jax.named_scope("wait_bar"):
        pl.semaphore_wait(barrier, chips)
    for ahead in range(planes):
        spread(ahead)
    get_up.start()
    for copy in small:
        copy.start()
    get_down.start()
    for t in range(early):
        get_edges(t).start()
    get_w2.start()
    get_edges(early).start()
    get_v1.start()
    get_v2.start()

    def local_row(index):
        owner, inner = index // (patches * owned), lax.rem(index, patches * owned)
        away = jnp.where(lax.rem(owner, 2) == core, 0, side)
        return owner // 2 * (patches * owned) + inner + away

    with jax.named_scope("wait_load"):
        get_nodes.wait()
        get_w1.wait()
    w_edge, w_send, w_recv = (w1.at[pl.ds(i * width, width)] for i in range(3))
    by_sender[...] = dot(win[own_rows, :], w_send[...]).astype(BF)
    by_receiver[...] = dot(win[own_rows, :], w_recv[...]).astype(BF)
    for copy in small:
        copy.wait()
    get_up.wait()
    up_pre[...] = (
        dot(ub[...], w_edge[...])
        + b1[...]
        + dot_t(one_hot_t(count, up_send[...]), by_sender[...])
    )
    blocks = TILE // 128
    index_rows = lambda t: pl.ds(pl.multiple_of(t * blocks, blocks), blocks)

    def main(t):
        get_edges(t).wait()
        pre[tile(t), :] = (
            dot(eb[tile(t), :], w_edge[...])
            + b1[...]
            + dot_t(one_hot_t(count, senders[index_rows(t), :] - RIM), by_sender[...])
            + dot_t(one_hot_t(count, receivers[index_rows(t), :]), by_receiver[...])
        )

    def early_step(t, carry):
        main(t)
        return carry

    def pass_on(ahead):
        with jax.named_scope("wait_spread"):
            settle(table.at[arriving(ahead)], spread_got.at[ahead])
        table_over(ahead).start()

    lax.fori_loop(0, early, early_step, 0)
    get_w2.wait()
    pass_on(0)
    pass_on(1)
    main(early)
    w2[...] = centred(w2[...])
    b2[...] = centred(b2[...])
    pass_on(2)
    pass_on(3)
    near, far = slice(0, side), slice(side, 2 * side)
    with jax.named_scope("up"):
        to_coarse = one_hot_t(2 * side, local_row(up_recv[...]))
        picked = dot_t(to_coarse[near], table[near, :])
        with jax.named_scope("wait_twin"):
            for ahead in range(planes):
                table_over(ahead).wait_recv()
        to_after.start()
        to_before.start()
        picked = (picked + dot_t(to_coarse[far], table[far, :])).astype(BF)
        new = tail(up_pre[...] + dot(picked, w_recv[...]), w2, b2, gain, shift)
        new = (ub[...].astype(F32) + new).astype(BF)
        ub[...] = new
        part[far, :] = dot(to_coarse[far], new).astype(BF)
        for ahead in range(planes):
            part_over(ahead).start()
        part[near, :] = dot(to_coarse[near], new).astype(BF)

    with jax.named_scope("home"):
        for ahead in range(planes):
            part_over(ahead).wait_recv()
            rows = ahead_rows(ahead)
            half[rows, :] = (part[rows, :].astype(F32) + beside[rows, :].astype(F32)).astype(BF)

            def home(other, device):
                block = pl.ds(pl.multiple_of(other * owned, owned), owned)
                remote(half.at[block], landed.at[mine], home_sent, home_got, device).start()

            in_plane(ahead, home)
        landed[mine, :] = half[mine, :]

    with jax.named_scope("down"):
        get_down.wait()
        picked = dot_t(one_hot_t(2 * side, local_row(down_send[...])), table[...]).astype(BF)
        to_fine = one_hot_t(count, down_recv[...])
        full = (
            dot(db[...], w_edge[...])
            + b1[...]
            + dot_t(to_fine, by_receiver[...])
            + dot(picked, w_send[...])
        )
        new = tail(full, w2, b2, gain, shift)
        new = (db[...].astype(F32) + new).astype(BF)
        db[...] = new
        sums[...] = dot(to_fine, new)

    with jax.named_scope("wait_rim"):
        to_after.wait_recv()
        to_before.wait_recv()
    by_rim[0:RIM, :] = dot(win[0:RIM, :], w_send[...]).astype(BF)
    by_rim[RIM:, :] = dot(win[RIM + count :, :], w_send[...]).astype(BF)

    def finished(t):
        send_row = senders[index_rows(t), :]
        rim_row = jnp.where(
            send_row < RIM, send_row, jnp.where(send_row < RIM + count, -1, send_row - count)
        )
        new = tail(
            pre[tile(t), :] + dot_t(one_hot_t(2 * RIM, rim_row), by_rim[...]), w2, b2, gain, shift
        )
        slot = lax.broadcasted_iota(jnp.int32, (TILE, 1), 0) + t * TILE
        return (eb[tile(t), :].astype(F32) + jnp.where(slot < live[0], new, 0.0)).astype(BF)

    def step(i, carry):
        first, second = finished(2 * i), finished(2 * i + 1)
        eb[tile(2 * i), :] = first
        eb[tile(2 * i + 1), :] = second
        rows = pl.ds(pl.multiple_of(2 * i * blocks, 2 * blocks), 2 * blocks)
        index = receivers[rows, :]
        slot = (
            lax.broadcasted_iota(jnp.int32, index.shape, 0) * 128
            + lax.broadcasted_iota(jnp.int32, index.shape, 1)
            + 2 * i * TILE
        )
        sums[...] += dot(
            one_hot_t(count, jnp.where(slot < live[0], index, -1)),
            jnp.concatenate([first, second], axis=0),
        )
        return carry

    with jax.named_scope("tails"):
        lax.fori_loop(0, steps // 2, step, 0)
    get_v1.wait()
    get_v2.wait()
    v2[...] = centred(v2[...])
    c2[...] = centred(c2[...])

    def node_net(old, summed):
        inner = dot(old, v1[0:width, :]) + c1[...] + dot(summed, v1[width : 2 * width, :])
        return (old.astype(F32) + tail(inner, v2, c2, node_gain, node_shift)).astype(BF)

    with jax.named_scope("node"):
        fine_new[...] = node_net(win[own_rows, :], sums[...].astype(BF))

    with jax.named_scope("wait_home"):
        settle(landed.at[all_but_one], home_got)
    with jax.named_scope("ends"):
        arrived = jnp.sum(landed[...].astype(F32).reshape(chips, owned, width), axis=0).astype(BF)
        coarse_new[...] = node_net(table[mine, :], arrived)
        to_after.wait_send()
        to_before.wait_send()
        settle(table.at[all_but_one], spread_sent)
        settle(half.at[all_but_one], home_sent)
        for ahead in range(planes):
            table_over(ahead).wait_send()
            part_over(ahead).wait_send()


def writer(fine, coarse, edges, up, down, *outs_and_sem):
    *outs, sem = outs_and_sem
    copies = []
    for source, target in zip((edges, fine, up, down, coarse), (outs[2], outs[0], *outs[3:], outs[1])):
        size = min(source.shape[0], 512)
        for at in range(0, source.shape[0], size):
            rows = pl.ds(at, size)
            copies.append(pltpu.make_async_copy(source.at[rows], target.at[rows], sem.at[len(copies)]))
    for copy in copies:
        copy.start()
    for copy in copies:
        copy.wait()


def body(
    fine_nodes, coarse_nodes, fine_edges, fine_senders, fine_receivers, fine_live,
    up_edges, up_senders, up_receivers, down_edges, down_senders, down_receivers,
    edge_in_weight, edge_in_bias, edge_out_weight, edge_out_bias, edge_gain, edge_shift,
    node_in_weight, node_in_bias, node_out_weight, node_out_bias, node_gain, node_shift,
):
    groups, patches = lax.axis_size("group"), lax.axis_size("patch")
    count, width = fine_nodes.shape
    owned = coarse_nodes.shape[0]
    slots = fine_edges.shape[0]
    crossing = up_edges.shape[0]
    everywhere = groups * patches * owned
    side = everywhere // 2
    steps = slots // TILE
    lanes = lambda index: index.reshape(-1, 128)
    row = lambda vector: vector.reshape(1, -1)
    vm = pl.BlockSpec(memory_space=pltpu.VMEM)
    anywhere = pl.BlockSpec(memory_space=pl.ANY)
    outs = (fine_nodes, coarse_nodes, fine_edges, up_edges, down_edges)
    rows = lambda n, dtype=BF: pltpu.VMEM((n, width), dtype)
    dma = pltpu.SemaphoreType.DMA
    indices = tuple(
        lanes(a)
        for a in (fine_senders, fine_receivers, up_senders, up_receivers, down_senders, down_receivers)
    )
    vectors = tuple(
        row(a)
        for a in (
            edge_in_bias, edge_out_bias, edge_gain, edge_shift,
            node_in_bias, node_out_bias, node_gain, node_shift,
        )
    )
    results = pl.pallas_call(
        functools.partial(kernel, groups, patches),
        out_shape=tuple(pltpu.VMEM(a.shape, a.dtype) for a in outs),
        in_specs=[anywhere] * 24,
        out_specs=(vm,) * 5,
        scratch_shapes=[
            rows(count + 2 * RIM),
            rows(3 * width), rows(width), rows(2 * width), rows(width),
            rows(count), rows(count), rows(slots, F32), rows(count, F32),
            rows(everywhere), rows(everywhere), rows(side), rows(side), rows(side),
            rows(crossing, F32),
            *(pltpu.VMEM(a.shape, a.dtype) for a in indices + vectors),
            rows(2 * RIM), pltpu.SMEM((1,), jnp.int32),
            dma((8 + steps,)), dma((len(indices + vectors) + 1,)), dma((2,)), dma((2,)),
            dma(()), dma((4,)), dma((8,)), dma((8,)), dma(()), dma(()),
        ],
        compiler_params=pltpu.CompilerParams(
            vmem_limit_bytes=50 * 1024 * 1024, collective_id=0, has_side_effects=True
        ),
    )(
        fine_live, *indices, *vectors,
        fine_nodes, coarse_nodes, fine_edges, up_edges, down_edges,
        edge_in_weight, edge_out_weight, node_in_weight, node_out_weight,
    )
    return pl.pallas_call(
        writer,
        out_shape=tuple(jax.ShapeDtypeStruct(a.shape, a.dtype) for a in outs),
        in_specs=[vm] * 5,
        out_specs=(anywhere,) * 5,
        scratch_shapes=[dma((slots // 512 + count // 512 + 3,))],
        compiler_params=pltpu.CompilerParams(vmem_limit_bytes=2**20),
    )(*results)


def solution(mesh):
    rows, vector = P(BOTH, None), P(BOTH)
    return jax.shard_map(
        body,
        mesh=mesh,
        in_specs=(rows,) * 3 + (vector,) * 3 + (rows, vector, vector) * 2 + (P(),) * 12,
        out_specs=(rows,) * 5,
        check_vma=False,
    )
```
